256 devices in a mesh: grp: 2 (over y), seq: 64 (over x, z), head: 2 (over core).
Axes of the slice: x: 4, y: 2, z: 16, core: 2. Of those that a mesh axis runs over, the one named last changes fastest.
The devices are a block of a 4x16x16 slice.
Arguments:
- query_rows: bfloat16 [16, 32, 128], P('grp', 'head'), parts along dimension 0, may hold values from -100 to 100
- cache_keys: bfloat16 [4096, 8, 128, 128], P(('grp', 'seq'), 'head'), parts along dimension 0, may hold values from -5 to 5
- cache_values: bfloat16 [4096, 8, 128, 128], P(('grp', 'seq'), 'head'), parts along dimension 0, may hold values from -6 to 6
- page_table: int32 [4096], P('grp'), parts along dimension 0, may hold values from 0 to 2047, as said below
- seq_lengths: int32 [16], P('grp'), parts along dimension 0, may hold values from 128 to 32768, as said below
Outputs:
- attended: bfloat16 [16, 32, 128], P('grp', 'head'), parts along dimension 0
The draws below stay inside these ranges and needn't reach their ends.
There are 2 independent parts, one for each index of `grp`. The reference program is written for one: setup_inputs(seed, part) draws one part's arguments, and reference() takes and returns one part's arrays. A program takes and returns all parts, laid end to end along the dimension named above; each array names one. Nothing has to cross between parts.
Inputs may be any that keep to these rules, and one draw needn't show every extreme that they name: `page_table`: entry b * 256 + j is the pool slot of page j of sequence b; slot s lies on index s // 32 of seq; every slot appears once. `seq_lengths`: some sequence has exactly 32768 tokens.
All inputs are finite; a program needn't handle non-finite values.
Results may differ from the reference program's by a relative error of at most 0.0029.
Values may be sent and summed in bfloat16 or wider, within the bound.
A program may use at most 64 MiB of HBM per device.

```python
import math
import jax
import jax.numpy as jnp
from jax import lax

H = 32
KVH = 8
HD = 128
PAGE = 128
BATCH = 8
POOL = 2048
MAXP = 256


def slot_layout(key):
    return jax.random.permutation(jax.random.fold_in(key, 7), POOL).astype(jnp.int32)


def draw_page_table(key, part):
    return slot_layout(key)


def draw_seq_lengths(key, part):
    drawn = jax.random.randint(jax.random.fold_in(key, 5), (BATCH,), PAGE, MAXP * PAGE + 1)
    return drawn.at[0].set(MAXP * PAGE).astype(jnp.int32)


def draw_query_rows(key, part):
    values = jnp.clip(3.0 * jax.random.normal(jax.random.fold_in(key, 13), (BATCH, H, HD), jnp.float32), -15.0, 15.0)
    return values.astype(jnp.bfloat16)


def draw_cache_keys(key, part):
    values = jnp.clip(jax.random.normal(jax.random.fold_in(key, 17), (POOL, KVH, PAGE, HD), jnp.float32), -5.0, 5.0)
    return values.astype(jnp.bfloat16)


def shard_levels(key, shape, pieces, low, high):
    factor_of, own = 1.0, jax.random.fold_in(key, 6)
    for axis_at, shards_of in pieces:
        draws = jnp.exp(jax.random.uniform(jax.random.fold_in(own, axis_at), (shards_of,), jnp.float32, low / len(pieces), high / len(pieces)))
        factor_of = factor_of * jnp.repeat(draws, shape[axis_at] // shards_of).reshape([-1 if axis == axis_at else 1 for axis in range(len(shape))])
    return factor_of


def scatter_about(stream_key, shape, scale, limit, shards=(), kind=jnp.bfloat16):
    result = scale * jax.random.normal(stream_key, shape, jnp.float32)
    if shards:
        result = result * shard_levels(stream_key, shape, shards, -0.22, 0.18)
    return jnp.clip(result, -limit, limit).astype(kind)


def setup_inputs(seed: int = 0, part: int = 0) -> dict:
    key_of = jax.random.split(jax.random.key(seed), 6)
    own_keys = jax.random.split(jax.random.fold_in(key_of[5], part), 6)
    return {
        "query_rows": draw_query_rows(jax.random.fold_in(jax.random.fold_in(key_of[5], part), 71), part),
        "cache_keys": draw_cache_keys(jax.random.fold_in(jax.random.fold_in(key_of[5], part), 71), part),
        "cache_values": scatter_about(own_keys[2], (POOL, KVH, PAGE, HD), 1.0, 6.0, ((0, 64), (1, 2))),
        "page_table": draw_page_table(jax.random.fold_in(jax.random.fold_in(key_of[5], part), 71), part),
        "seq_lengths": draw_seq_lengths(jax.random.fold_in(jax.random.fold_in(key_of[5], part), 71), part),
    }


def reference(query_rows, cache_keys, cache_values, page_table, seq_lengths):
    group_size = H // KVH
    score_scale = 1.0 / math.sqrt(HD)
    positions = jnp.arange(MAXP * PAGE, dtype=jnp.int32)

    def per_sequence(seq_index):
        slots = lax.dynamic_slice_in_dim(page_table, (seq_index * MAXP).astype(jnp.int32), MAXP)
        keys_here = jnp.take(cache_keys, slots, axis=0).astype(jnp.float32)
        keys_here = keys_here.transpose(1, 0, 2, 3).reshape(KVH, MAXP * PAGE, HD)
        values_here = jnp.take(cache_values, slots, axis=0).astype(jnp.float32)
        values_here = values_here.transpose(1, 0, 2, 3).reshape(KVH, MAXP * PAGE, HD)
        queries = query_rows[seq_index].astype(jnp.float32).reshape(KVH, group_size, HD)
        scores = jnp.einsum('gqd,gpd->gqp', queries, keys_here, precision=lax.Precision.HIGHEST) * score_scale
        is_live = positions < seq_lengths[seq_index]
        row_top = lax.optimization_barrier(jnp.max(jnp.where(is_live, scores, -jnp.inf), axis=-1, keepdims=True))
        weights = jnp.where(is_live, jnp.exp(scores - row_top), 0.0)
        totals = lax.optimization_barrier(jnp.sum(weights, axis=-1))
        rounded = lax.optimization_barrier(weights.astype(jnp.bfloat16)).astype(jnp.float32)
        numerators = jnp.einsum('gqp,gpd->gqd', rounded, values_here, precision=lax.Precision.HIGHEST)
        return (numerators / totals[..., None]).reshape(H, HD).astype(jnp.bfloat16)
    return lax.map(per_sequence, jnp.arange(BATCH, dtype=jnp.int32))
```

```python
import functools
import math

import jax
import jax.numpy as jnp
from jax import lax
from jax.experimental import pallas as pl
from jax.experimental.pallas import tpu as pltpu
from jax.sharding import PartitionSpec as P

MESH = pl.DeviceIdType.MESH
NX, NZ = 4, 16
PAIR = 2
VERY_LOW = -1e30


def remote(src, dst, send, recv, seq):
    return pltpu.make_async_remote_copy(
        src_ref=src,
        dst_ref=dst,
        send_sem=send,
        recv_sem=recv,
        device_id={"seq": seq},
        device_id_type=MESH,
    )


def to_column(row, rows):
    lane = lax.broadcasted_iota(jnp.int32, (rows, row.shape[1]), 1)
    sub = lax.broadcasted_iota(jnp.int32, (rows, row.shape[1]), 0)
    return jnp.sum(jnp.where(lane == sub, row, 0.0), axis=1, keepdims=True)


def merged(parts, rows):
    tops = [p[rows : rows + 1] for p in parts]
    top = functools.reduce(jnp.maximum, tops)
    total, numer = None, None
    for p, t in zip(parts, tops):
        factor = jnp.exp2(t - top)
        tot = p[rows + 1 : rows + 2] * factor
        num = p[:rows] * to_column(factor, rows)
        total = tot if total is None else total + tot
        numer = num if numer is None else numer + num
    return numer, top, total


def kernel(
    q_hbm, k_hbm, v_hbm, table_hbm, len_ref, out_ref,
    q_buf, q_f32, k_buf, v_buf, table_buf, bias, scores, probs,
    part, mid, share, recv1, recv2, recv3,
    load_sem, k_sem, v_sem, send1, sem1, send2, sem2, send3, sem3,
):
    slots, kv, page, dim = k_hbm.shape
    batch, heads, _ = q_hbm.shape
    group = heads // kv
    table_rows = table_hbm.shape[0] // batch
    rows = part.shape[1]

    load_q = pltpu.make_async_copy(q_hbm, q_buf, load_sem.at[0])
    load_t = pltpu.make_async_copy(table_hbm, table_buf, load_sem.at[1])
    load_q.start()
    load_t.start()
    loads_k = [pltpu.make_async_copy(k_hbm.at[:, g], k_buf.at[g], k_sem.at[g]) for g in range(kv)]
    loads_v = [pltpu.make_async_copy(v_hbm.at[:, g], v_buf.at[g], v_sem.at[g]) for g in range(kv)]
    for g in range(kv):
        loads_k[g].start()
        loads_v[g].start()

    me = lax.axis_index("seq")
    x, z = me // NZ, me % NZ
    peers = NX * PAIR
    mine = x * PAIR + z % PAIR
    z_base = (z // PAIR) * PAIR
    chunk = [(mine + i) % peers for i in range(peers)]
    near = [(c // PAIR) * NZ + z_base + c % PAIR for c in chunk]
    far = [x * NZ + (z + PAIR * i) % NZ for i in range(NZ // PAIR)]

    barrier = pltpu.get_barrier_semaphore()
    others = near[1:] + far[1:]
    for other in others:
        pl.semaphore_signal(barrier, inc=1, device_id={"seq": other}, device_id_type=MESH)

    load_t.wait()
    first = me * slots
    lane = lax.broadcasted_iota(jnp.int32, (batch, page), 1)
    sub = lax.broadcasted_iota(jnp.int32, (batch, page), 0)
    length = jnp.zeros((batch, page), jnp.int32)
    for b in range(batch):
        length = jnp.where(sub == b, len_ref[b], length)
    tables = [table_buf[pl.ds(r, batch, stride=table_rows), :] for r in range(table_rows)]
    spans = [(length - page * (lane + page * r)).astype(jnp.float32) for r in range(table_rows)]
    lane_f32 = lane.astype(jnp.float32)
    for s in range(slots):
        found = functools.reduce(
            jnp.add, [jnp.where(t == first + s, n, 0.0) for t, n in zip(tables, spans)]
        )
        live = jnp.sum(found, axis=1, keepdims=True)
        bias[s] = jnp.where(lane_f32 < live, 0.0, VERY_LOW)

    load_q.wait()
    q_f32[...] = q_buf[...].astype(jnp.float32).reshape(batch * heads, dim)

    factor = math.log2(math.e) / math.sqrt(dim)
    tops = jnp.zeros((batch, page), jnp.float32)
    totals = jnp.zeros((batch, page), jnp.float32)
    for g in range(kv):
        query = jnp.concatenate(
            [q_f32[pl.ds(group * g + i, batch, stride=heads), :] for i in range(group)], axis=0
        ).astype(jnp.bfloat16)
        loads_k[g].wait()
        best = None
        for s in range(0, slots, 2):
            keys = k_buf[g, s : s + 2].reshape(2 * page, dim)
            got = lax.dot_general(
                query, keys, (((1,), (1,)), ((), ())), preferred_element_type=jnp.float32
            )
            for u in range(2):
                add = jnp.concatenate([bias[s + u]] * group, axis=0)
                now = got[:, u * page : (u + 1) * page] * factor + add
                scores[:, (s + u) * page : (s + u + 1) * page] = now
                best = now if best is None else jnp.maximum(best, now)
        top = jnp.max(best, axis=1, keepdims=True)
        total = jnp.zeros((group * batch, page), jnp.float32)
        for s in range(slots):
            p = jnp.exp2(scores[:, s * page : (s + 1) * page] - top)
            total = total + p
            probs[:, s * page : (s + 1) * page] = p.astype(jnp.bfloat16)
        total = jnp.sum(total, axis=1, keepdims=True)
        loads_v[g].wait()
        numer = jnp.dot(
            probs[...], v_buf[g].reshape(slots * page, dim), preferred_element_type=jnp.float32
        )
        for i in range(group):
            h = group * g + i
            own = slice(i * batch, (i + 1) * batch)
            part[:, h, :] = numer[own]
            tops = jnp.where(lane == h, top[own], tops)
            totals = jnp.where(lane == h, total[own], totals)
    part[:, heads, :] = tops
    part[:, heads + 1, :] = totals

    pl.semaphore_wait(barrier, len(others))

    copies = [
        remote(part.at[chunk[i]], recv1.at[i - 1], send1.at[i - 1], sem1.at[i - 1], near[i])
        for i in range(1, peers)
    ]
    for c in copies:
        c.start()
    own = part[mine]
    for c in copies:
        c.wait_recv()
    numer, top, total = merged([own] + [recv1[i] for i in range(peers - 1)], heads)
    mid[0:heads] = numer
    mid[heads : heads + 1] = top
    mid[heads + 1 : heads + 2] = total

    copies2 = [
        remote(mid, recv2.at[i - 1], send2.at[i - 1], sem2.at[i - 1], far[i])
        for i in range(1, NZ // PAIR)
    ]
    for c in copies2:
        c.start()
    own = mid[...]
    for c in copies2:
        c.wait_recv()
    numer, top, total = merged([own] + [recv2[i] for i in range(NZ // PAIR - 1)], heads)
    share[...] = (numer / to_column(total, heads)).astype(jnp.bfloat16)

    copies3 = [
        remote(share, recv3.at[i - 1], send3.at[i - 1], sem3.at[i - 1], near[i])
        for i in range(1, peers)
    ]
    for c in copies3:
        c.start()
    out_ref[mine] = share[...]
    for i, c in enumerate(copies3):
        c.wait_recv()
        out_ref[(mine + peers - 1 - i) % peers] = recv3[i]
    for c in copies + copies2 + copies3:
        c.wait_send()


def shards(query_rows, cache_keys, cache_values, page_table, seq_lengths):
    slots, kv, page, dim = cache_keys.shape
    batch, heads, _ = query_rows.shape
    peers, fars = NX * PAIR, NZ // PAIR
    rows = heads + 8
    dma = pltpu.SemaphoreType.DMA
    return pl.pallas_call(
        kernel,
        out_shape=jax.ShapeDtypeStruct(query_rows.shape, query_rows.dtype),
        in_specs=[pl.BlockSpec(memory_space=pl.ANY)] * 4
        + [pl.BlockSpec(memory_space=pltpu.SMEM)],
        out_specs=pl.BlockSpec(memory_space=pltpu.VMEM),
        scratch_shapes=[
            pltpu.VMEM(query_rows.shape, query_rows.dtype),
            pltpu.VMEM((batch * heads, dim), jnp.float32),
            pltpu.VMEM((kv, slots, page, dim), cache_keys.dtype),
            pltpu.VMEM((kv, slots, page, dim), cache_values.dtype),
            pltpu.VMEM((page_table.shape[0] // page, page), jnp.int32),
            pltpu.VMEM((slots, batch, page), jnp.float32),
            pltpu.VMEM((heads // kv * batch, slots * page), jnp.float32),
            pltpu.VMEM((heads // kv * batch, slots * page), jnp.bfloat16),
            pltpu.VMEM((batch, rows, dim), jnp.float32),
            pltpu.VMEM((rows, dim), jnp.float32),
            pltpu.VMEM((heads, dim), jnp.bfloat16),
            pltpu.VMEM((peers - 1, rows, dim), jnp.float32),
            pltpu.VMEM((fars - 1, rows, dim), jnp.float32),
            pltpu.VMEM((peers - 1, heads, dim), jnp.bfloat16),
            dma((2,)),
            dma((kv,)),
            dma((kv,)),
            dma((peers - 1,)),
            dma((peers - 1,)),
            dma((fars - 1,)),
            dma((fars - 1,)),
            dma((peers - 1,)),
            dma((peers - 1,)),
        ],
        compiler_params=pltpu.CompilerParams(collective_id=0, has_side_effects=True),
        name="attend",
    )(query_rows, cache_keys, cache_values, page_table.reshape(-1, page), seq_lengths)


def solution(mesh):
    return jax.shard_map(
        shards,
        mesh=mesh,
        in_specs=(
            P("grp", "head", None),
            P(("grp", "seq"), "head", None, None),
            P(("grp", "seq"), "head", None, None),
            P("grp"),
            P("grp"),
        ),
        out_specs=P("grp", "head", None),
        check_vma=False,
    )
```

```python
import functools
import math

import jax
import jax.numpy as jnp
from jax import lax
from jax.experimental import pallas as pl
from jax.experimental.pallas import tpu as pltpu
from jax.sharding import PartitionSpec as P

MESH = pl.DeviceIdType.MESH
NX, NZ = 4, 16
LATE = 12
VERY_LOW = -1e30
LEVELS = 32767.0


def remote(src, dst, send, recv, seq):
    return pltpu.make_async_remote_copy(
        src_ref=src,
        dst_ref=dst,
        send_sem=send,
        recv_sem=recv,
        device_id={"seq": seq},
        device_id_type=MESH,
    )


def diagonal(rows, lanes, first):
    lane = lax.broadcasted_iota(jnp.int32, (rows, lanes), 1)
    sub = lax.broadcasted_iota(jnp.int32, (rows, lanes), 0)
    return lane == sub + first


def to_column(row, rows):
    return jnp.sum(jnp.where(diagonal(rows, row.shape[1], 0), row, 0.0), axis=1, keepdims=True)


def kernel(
    q_hbm, k_hbm, v_hbm, table_hbm, len_ref, out_ref,
    q_buf, q_f32, k_buf, v_buf, table_buf, bias, scores, probs,
    numer16, stats, recv16, recv_stats, total_numer, total_row, top_row, finished, fin_f32,
    load_sem, k_sem, v_sem, send_n, send_s, recv_n, recv_s, send_f, recv_f,
):
    slots, kv, page, dim = k_hbm.shape
    batch, heads, _ = q_hbm.shape
    group = heads // kv
    table_rows = table_hbm.shape[0] // batch
    rows = group * batch

    load_q = pltpu.make_async_copy(q_hbm, q_buf, load_sem.at[0])
    load_t = pltpu.make_async_copy(table_hbm, table_buf, load_sem.at[1])
    load_q.start()
    load_t.start()
    loads_k = [pltpu.make_async_copy(k_hbm.at[:, g], k_buf.at[g], k_sem.at[g]) for g in range(kv)]
    loads_v = [pltpu.make_async_copy(v_hbm.at[:, g], v_buf.at[g], v_sem.at[g]) for g in range(kv)]
    for g in range(kv):
        loads_k[g].start()
        loads_v[g].start()

    me = lax.axis_index("seq")
    mine, z = me // NZ, me % NZ
    owner = z == 0
    owners = [g * NZ for g in range(kv)]

    barrier = pltpu.get_barrier_semaphore()

    @pl.when(owner)
    def _():
        @pl.loop(1, NX * NZ)
        def _(i):
            other = (me + i) % (NX * NZ)
            pl.semaphore_signal(barrier, inc=1, device_id={"seq": other}, device_id_type=MESH)

    @pl.when(jnp.logical_not(owner))
    def _():
        for other in owners:
            pl.semaphore_signal(barrier, inc=1, device_id={"seq": other}, device_id_type=MESH)

    load_t.wait()
    first = me * slots
    lane = lax.broadcasted_iota(jnp.int32, (batch, page), 1)
    sub = lax.broadcasted_iota(jnp.int32, (batch, page), 0)
    length = jnp.zeros((batch, page), jnp.int32)
    for b in range(batch):
        length = jnp.where(sub == b, len_ref[b], length)
    tables = [table_buf[pl.ds(r, batch, stride=table_rows), :] for r in range(table_rows)]
    spans = [(length - page * (lane + page * r)).astype(jnp.float32) for r in range(table_rows)]
    lane_f32 = lane.astype(jnp.float32)
    for s in range(slots):
        found = functools.reduce(
            jnp.add, [jnp.where(t == first + s, n, 0.0) for t, n in zip(tables, spans)]
        )
        live = jnp.sum(found, axis=1, keepdims=True)
        bias[s] = jnp.where(lane_f32 < live, 0.0, VERY_LOW)

    load_q.wait()
    q_f32[...] = q_buf[...].astype(jnp.float32).reshape(batch * heads, dim)

    factor = math.log2(math.e) / math.sqrt(dim)

    def sends(g):
        return (
            remote(numer16.at[g], recv16.at[me], send_n.at[g], recv_n.at[me], owners[g]),
            remote(stats.at[g], recv_stats.at[me], send_s.at[g], recv_s.at[me], owners[g]),
        )

    @pl.when(jnp.logical_not(owner))
    def _():
        pl.semaphore_wait(barrier, NX)

    for g in range(kv):
        query = jnp.concatenate(
            [q_f32[pl.ds(group * g + i, batch, stride=heads), :] for i in range(group)], axis=0
        ).astype(jnp.bfloat16)
        loads_k[g].wait()
        best = None
        for s in range(0, slots, 2):
            keys = k_buf[g, s : s + 2].reshape(2 * page, dim)
            got = lax.dot_general(
                query, keys, (((1,), (1,)), ((), ())), preferred_element_type=jnp.float32
            )
            for u in range(2):
                add = jnp.concatenate([bias[s + u]] * group, axis=0)
                now = got[:, u * page : (u + 1) * page] * factor + add
                scores[:, (s + u) * page : (s + u + 1) * page] = now
                best = now if best is None else jnp.maximum(best, now)
        top = jnp.max(best, axis=1, keepdims=True)
        total = jnp.zeros((rows, page), jnp.float32)
        for s in range(slots):
            p = jnp.exp2(scores[:, s * page : (s + 1) * page] - top)
            total = total + p
            probs[:, s * page : (s + 1) * page] = p.astype(jnp.bfloat16)
        total = jnp.sum(total, axis=1, keepdims=True)
        loads_v[g].wait()
        numer = jnp.dot(
            probs[...], v_buf[g].reshape(slots * page, dim), preferred_element_type=jnp.float32
        )
        largest = jnp.max(jnp.abs(numer), axis=1, keepdims=True)
        steps = numer * (LEVELS / jnp.maximum(largest, 1e-30))
        numer16[g] = jnp.floor(steps + 0.5).astype(jnp.int32).astype(jnp.int16)
        row = sum(
            jnp.where(diagonal(rows, dim, i * rows), column, 0.0)
            for i, column in enumerate((top, total, largest * (1.0 / LEVELS)))
        )
        stats[g] = jnp.sum(row, axis=0, keepdims=True)

        @pl.when(jnp.logical_not(owner))
        def _():
            for c in sends(g):
                c.start()

    @pl.when(owner)
    def _():
        pl.semaphore_wait(barrier, NX * NZ - 1)
        for g in range(kv):

            @pl.when(mine != g)
            def _():
                for c in sends(g):
                    c.start()

        recv16[me] = numer16[mine]
        recv_stats[me] = stats[mine]
        total_numer[...] = jnp.zeros_like(total_numer)
        total_row[...] = jnp.zeros_like(total_row)
        top_row[...] = jnp.full_like(top_row, VERY_LOW)

        def add(zz):
            sources = [xx * NZ + zz for xx in range(NX)]
            for src in sources:

                @pl.when(src != me)
                def _():
                    remote(numer16.at[0], recv16.at[src], send_n.at[0], recv_n.at[src], 0).wait_recv()
                    remote(stats.at[0], recv_stats.at[src], send_s.at[0], recv_s.at[src], 0).wait_recv()

            got = jnp.concatenate([recv_stats[src] for src in sources] * 2, axis=0)
            totals = pltpu.roll(got, dim - rows, 1)
            scales = pltpu.roll(got, dim - 2 * rows, 1)
            before = top_row[...]
            top = jnp.maximum(before, jnp.max(got, axis=0, keepdims=True))
            weight = jnp.exp2(got - top)
            keep = jnp.exp2(before - top)
            top_row[...] = top
            both = weight * totals
            new_total = total_row[...] * keep
            for i in range(NX):
                new_total = new_total + both[i : i + 1]
            total_row[...] = new_total
            scaled = weight * scales
            numer = total_numer[...] * to_column(keep, rows)
            for i, src in enumerate(sources):
                numer = numer + recv16[src].astype(jnp.int32).astype(jnp.float32) * to_column(
                    scaled[i : i + 1], rows
                )
            total_numer[...] = numer

        @pl.loop(1, LATE)
        def _(zz):
            add(zz)

        add(0)

        @pl.loop(LATE, NZ)
        def _(zz):
            add(zz)

        done = total_numer[...] / to_column(total_row[...], rows)
        finished[mine] = done.astype(finished.dtype)

        @pl.loop(0, NZ)
        def _(zz):
            for xx in range(NX):
                other = xx * NZ + zz

                @pl.when(other != me)
                def _():
                    remote(
                        finished.at[mine], finished.at[mine], send_f.at[other], recv_f.at[mine], other
                    ).start()

    for g in range(kv):

        @pl.when(me != owners[g])
        def _():
            remote(finished.at[g], finished.at[g], send_f.at[0], recv_f.at[g], 0).wait_recv()

    fin_f32[...] = finished[...].astype(jnp.float32).reshape(heads * batch, dim)
    for b in range(batch):
        out_ref[b] = fin_f32[pl.ds(b, heads, stride=batch), :].astype(out_ref.dtype)

    for g in range(kv):

        @pl.when(me != owners[g])
        def _():
            for c in sends(g):
                c.wait_send()

    @pl.when(owner)
    def _():
        @pl.loop(0, NX * NZ)
        def _(other):
            @pl.when(other != me)
            def _():
                remote(
                    finished.at[mine], finished.at[mine], send_f.at[other], recv_f.at[mine], other
                ).wait_send()


def shards(query_rows, cache_keys, cache_values, page_table, seq_lengths):
    slots, kv, page, dim = cache_keys.shape
    batch, heads, _ = query_rows.shape
    rows = heads // kv * batch
    devices = NX * NZ
    dma = pltpu.SemaphoreType.DMA
    return pl.pallas_call(
        kernel,
        out_shape=jax.ShapeDtypeStruct(query_rows.shape, query_rows.dtype),
        in_specs=[pl.BlockSpec(memory_space=pltpu.HBM)] * 4
        + [pl.BlockSpec(memory_space=pltpu.SMEM)],
        out_specs=pl.BlockSpec(memory_space=pltpu.VMEM),
        scratch_shapes=[
            pltpu.VMEM(query_rows.shape, query_rows.dtype),
            pltpu.VMEM((batch * heads, dim), jnp.float32),
            pltpu.VMEM((kv, slots, page, dim), cache_keys.dtype),
            pltpu.VMEM((kv, slots, page, dim), cache_values.dtype),
            pltpu.VMEM((page_table.shape[0] // page, page), jnp.int32),
            pltpu.VMEM((slots, batch, page), jnp.float32),
            pltpu.VMEM((rows, slots * page), jnp.float32),
            pltpu.VMEM((rows, slots * page), jnp.bfloat16),
            pltpu.VMEM((kv, rows, dim), jnp.int16),
            pltpu.VMEM((kv, 1, dim), jnp.float32),
            pltpu.VMEM((devices, rows, dim), jnp.int16),
            pltpu.VMEM((devices, 1, dim), jnp.float32),
            pltpu.VMEM((rows, dim), jnp.float32),
            pltpu.VMEM((1, dim), jnp.float32),
            pltpu.VMEM((1, dim), jnp.float32),
            pltpu.VMEM((kv, rows, dim), query_rows.dtype),
            pltpu.VMEM((heads * batch, dim), jnp.float32),
            dma((2,)),
            dma((kv,)),
            dma((kv,)),
            dma((kv,)),
            dma((kv,)),
            dma((devices,)),
            dma((devices,)),
            dma((devices,)),
            dma((kv,)),
        ],
        compiler_params=pltpu.CompilerParams(
            collective_id=0, has_side_effects=True, vmem_limit_bytes=56 << 20
        ),
        name="attend",
    )(query_rows, cache_keys, cache_values, page_table.reshape(-1, page), seq_lengths)


def solution(mesh):
    return jax.shard_map(
        shards,
        mesh=mesh,
        in_specs=(
            P("grp", "head", None),
            P(("grp", "seq"), "head", None, None),
            P(("grp", "seq"), "head", None, None),
            P("grp"),
            P("grp"),
        ),
        out_specs=P("grp", "head", None),
        check_vma=False,
    )
```

```python
import functools
import math

import jax
import jax.numpy as jnp
from jax import lax
from jax.experimental import pallas as pl
from jax.experimental.pallas import tpu as pltpu
from jax.sharding import PartitionSpec as P

MESH = pl.DeviceIdType.MESH
NX, NZ = 4, 16
OWNER = 1
NEAR = 3
RELAY = 5
LATE = 13
VERY_LOW = -1e30
LEVELS = 32767.0


def remote(src, dst, send, recv, seq):
    return pltpu.make_async_remote_copy(
        src_ref=src,
        dst_ref=dst,
        send_sem=send,
        recv_sem=recv,
        device_id={"seq": seq},
        device_id_type=MESH,
    )


def diagonal(rows, lanes, first):
    lane = lax.broadcasted_iota(jnp.int32, (rows, lanes), 1)
    sub = lax.broadcasted_iota(jnp.int32, (rows, lanes), 0)
    return lane == sub + first


def to_column(row, rows):
    return jnp.sum(jnp.where(diagonal(rows, row.shape[1], 0), row, 0.0), axis=1, keepdims=True)


def kernel(
    q_hbm, k_hbm, v_hbm, table_hbm, len_hbm, out_ref,
    len_buf, q_buf, q_f32, k_buf, v_buf, table_buf, bias, scores, probs,
    numer16, stats, recv16, recv_stats, total_numer, total_row, top_row, finished, fin_f32,
    load_sem, k_sem, v_sem, send_n, send_s, recv_n, recv_s, send_f, recv_f, send_w, recv_w, ready,
):
    slots, kv, page, dim = k_hbm.shape
    batch, heads, _ = q_hbm.shape
    group = heads // kv
    table_rows = table_hbm.shape[0] // batch
    rows = group * batch
    pairs = [(g, g + 1) for g in range(0, kv, 2)]
    devices = NX * NZ

    load_t = pltpu.make_async_copy(table_hbm, table_buf, load_sem.at[0])
    load_l = pltpu.make_async_copy(len_hbm, len_buf, load_sem.at[1])
    load_q = pltpu.make_async_copy(q_hbm, q_buf, load_sem.at[2])
    loads_k = [pltpu.make_async_copy(k_hbm.at[:, g], k_buf.at[g], k_sem.at[g]) for g in range(kv)]
    loads_v = [pltpu.make_async_copy(v_hbm.at[:, g], v_buf.at[g], v_sem.at[g]) for g in range(kv)]
    load_t.start()
    load_l.start()
    load_q.start()
    for c in loads_k:
        c.start()

    me = lax.axis_index("seq")
    x, z = me // NZ, me % NZ
    owner = z == OWNER
    relay = z == RELAY
    fed = jnp.logical_and(z > NEAR, jnp.logical_not(relay))
    owners = [g * NZ + OWNER for g in range(kv)]
    column = [zz for zz in range(NEAR + 1, NZ) if zz != RELAY]

    barrier = pltpu.get_barrier_semaphore()

    def signal(sem, other):
        pl.semaphore_signal(sem, inc=1, device_id={"seq": other}, device_id_type=MESH)

    @pl.when(owner)
    def _():
        @pl.loop(1, devices)
        def _(i):
            signal(barrier, (me + i) % devices)

    @pl.when(jnp.logical_not(owner))
    def _():
        for other in owners:
            signal(barrier, other)

    @pl.when(relay)
    def _():
        for zz in column:
            signal(barrier, x * NZ + zz)

    with jax.named_scope("tw"):
        load_t.wait()
        load_l.wait()
        load_q.wait()
    for c in loads_v:
        c.start()
    first = me * slots
    lane = lax.broadcasted_iota(jnp.int32, (batch, page), 1)
    sub = lax.broadcasted_iota(jnp.int32, (batch, page), 0)
    length = jnp.zeros((batch, page), jnp.int32)
    for b in range(batch):
        length = jnp.where(sub == b, len_buf[b], length)
    tables = [table_buf[pl.ds(r, batch, stride=table_rows), :] for r in range(table_rows)]
    spans = [(length - page * (lane + page * r)).astype(jnp.float32) for r in range(table_rows)]
    lane_f32 = lane.astype(jnp.float32)
    for s in range(slots):
        found = functools.reduce(
            jnp.add, [jnp.where(t == first + s, n, 0.0) for t, n in zip(tables, spans)]
        )
        live = jnp.sum(found, axis=1, keepdims=True)
        bias[s] = jnp.where(lane_f32 < live, 0.0, VERY_LOW)
    q_f32[...] = q_buf[...].astype(jnp.float32).reshape(batch * heads, dim)

    factor = math.log2(math.e) / math.sqrt(dim)

    def sends(g):
        return (
            remote(numer16.at[g], recv16.at[me], send_n.at[g], recv_n.at[me], owners[g]),
            remote(stats.at[g], recv_stats.at[me], send_s.at[g], recv_s.at[me], owners[g]),
        )

    columns = []
    for p, pair in enumerate(pairs):
        blocks = []
        for i, g in enumerate(pair):
            query = jnp.concatenate(
                [q_f32[pl.ds(group * g + j, batch, stride=heads), :] for j in range(group)], axis=0
            ).astype(jnp.bfloat16)
            empty = jnp.zeros_like(query)
            blocks.append(jnp.concatenate([empty] * i + [query] + [empty] * (1 - i), axis=1))
        query = jnp.concatenate(blocks, axis=0)
        with jax.named_scope(f"kw{p}"):
            for g in pair:
                loads_k[g].wait()
        best = None
        for s in range(0, slots, 2):
            keys = jnp.concatenate(
                [k_buf[g, s : s + 2].reshape(2 * page, dim) for g in pair], axis=1
            )
            got = lax.dot_general(
                query, keys, (((1,), (1,)), ((), ())), preferred_element_type=jnp.float32
            )
            for u in range(2):
                add = jnp.concatenate([bias[s + u]] * (2 * group), axis=0)
                now = got[:, u * page : (u + 1) * page] * factor + add
                scores[p, :, (s + u) * page : (s + u + 1) * page] = now
                best = now if best is None else jnp.maximum(best, now)
        top = jnp.max(best, axis=1, keepdims=True)
        total = jnp.zeros((2 * rows, page), jnp.float32)
        for s in range(slots):
            w = jnp.exp2(scores[p, :, s * page : (s + 1) * page] - top)
            total = total + w
            probs[p, :, s * page : (s + 1) * page] = w.astype(jnp.bfloat16)
        columns.append((top, jnp.sum(total, axis=1, keepdims=True)))

    with jax.named_scope("bw"):

        @pl.when(fed)
        def _():
            pl.semaphore_wait(barrier, kv + 1)
            signal(ready, x * NZ + RELAY)

        @pl.when(jnp.logical_not(jnp.logical_or(owner, fed)))
        def _():
            pl.semaphore_wait(barrier, kv)

    for p, pair in enumerate(pairs):
        with jax.named_scope(f"vw{p}"):
            for g in pair:
                loads_v[g].wait()
        numers = jnp.zeros((2 * rows, 2 * dim), jnp.float32)
        for s in range(0, slots, 2):
            values = jnp.concatenate(
                [v_buf[g, s : s + 2].reshape(2 * page, dim) for g in pair], axis=1
            )
            numers = numers + jnp.dot(
                probs[p, :, s * page : (s + 2) * page], values, preferred_element_type=jnp.float32
            )
        for i, g in enumerate(pair):
            own = slice(i * rows, (i + 1) * rows)
            numer = numers[own, i * dim : (i + 1) * dim]
            largest = jnp.max(jnp.abs(numer), axis=1, keepdims=True)
            steps = numer * (LEVELS / jnp.maximum(largest, 1e-30))
            numer16[g] = jnp.floor(steps + 0.5).astype(jnp.int32).astype(jnp.int16)
            top, total = columns[p]
            row = sum(
                jnp.where(diagonal(rows, dim, j * rows), c, 0.0)
                for j, c in enumerate((top[own], total[own], largest * (1.0 / LEVELS)))
            )
            stats[g] = jnp.sum(row, axis=0, keepdims=True)

        @pl.when(jnp.logical_not(owner))
        def _():
            with jax.named_scope(f"snd{p}"):
                for g in pair:
                    for c in sends(g):
                        c.start()

    def near(zz, xx):
        other = xx * NZ + zz
        return remote(
            finished.at[x], finished.at[x], send_f.at[xx * (NEAR + 2) + min(zz, NEAR + 1)], recv_f.at[x], other
        )

    near_z = [OWNER] + [zz for zz in range(NEAR + 1) if zz != OWNER] + [RELAY]

    @pl.when(owner)
    def _():
        with jax.named_scope("bar"):
            pl.semaphore_wait(barrier, devices - 1)
        for g in range(kv):

            @pl.when(x != g)
            def _():
                for c in sends(g):
                    c.start()

        recv16[me] = numer16[x]
        recv_stats[me] = stats[x]
        total_numer[...] = jnp.zeros_like(total_numer)
        total_row[...] = jnp.zeros_like(total_row)
        top_row[...] = jnp.full_like(top_row, VERY_LOW)

        def add(zz):
            sources = [xx * NZ + zz for xx in range(NX)]
            with jax.named_scope("rw"):
                for src in sources:

                    @pl.when(src != me)
                    def _():
                        remote(numer16.at[0], recv16.at[src], send_n.at[0], recv_n.at[src], 0).wait_recv()
                        remote(stats.at[0], recv_stats.at[src], send_s.at[0], recv_s.at[src], 0).wait_recv()

            got = jnp.concatenate([recv_stats[src] for src in sources] * 2, axis=0)
            totals = pltpu.roll(got, dim - rows, 1)
            scales = pltpu.roll(got, dim - 2 * rows, 1)
            before = top_row[...]
            top = jnp.maximum(before, jnp.max(got, axis=0, keepdims=True))
            weight = jnp.exp2(got - top)
            keep = jnp.exp2(before - top)
            top_row[...] = top
            both = weight * totals
            new_total = total_row[...] * keep
            for i in range(NX):
                new_total = new_total + both[i : i + 1]
            total_row[...] = new_total
            scaled = weight * scales
            numer = total_numer[...] * to_column(keep, rows)
            for i, src in enumerate(sources):
                numer = numer + recv16[src].astype(jnp.int32).astype(jnp.float32) * to_column(
                    scaled[i : i + 1], rows
                )
            total_numer[...] = numer

        @pl.loop(OWNER + 1, LATE)
        def _(zz):
            add(zz)

        @pl.loop(0, OWNER + 1)
        def _(zz):
            add(OWNER - zz)

        @pl.loop(LATE, NZ)
        def _(zz):
            add(zz)

        done = total_numer[...] / to_column(total_row[...], rows)
        finished[x] = done.astype(finished.dtype)
        with jax.named_scope("bcast"):
            for zz in near_z:
                for xx in range(NX):
                    if zz == OWNER:

                        @pl.when(x != xx)
                        def _():
                            near(zz, xx).start()
                    else:
                        near(zz, xx).start()

    @pl.when(jnp.logical_not(fed))
    def _():
        for g in range(kv):

            @pl.when(me != owners[g])
            def _():
                with jax.named_scope(f"fw{g}"):
                    remote(finished.at[g], finished.at[g], send_f.at[0], recv_f.at[g], 0).wait_recv()

    def forward(i):
        return remote(finished, finished, send_w.at[i], recv_w, x * NZ + column[i])

    @pl.when(fed)
    def _():
        with jax.named_scope("fww"):
            forward(0).wait_recv()

    @pl.when(relay)
    def _():
        pl.semaphore_wait(ready, len(column))
        for i in range(len(column)):
            forward(i).start()

    fin_f32[...] = finished[...].astype(jnp.float32).reshape(heads * batch, dim)
    for b in range(batch):
        out_ref[b] = fin_f32[pl.ds(b, heads, stride=batch), :].astype(out_ref.dtype)

    with jax.named_scope("ws"):
        for g in range(kv):

            @pl.when(me != owners[g])
            def _():
                for c in sends(g):
                    c.wait_send()

        @pl.when(owner)
        def _():
            for zz in near_z:
                for xx in range(NX):
                    if zz == OWNER:

                        @pl.when(x != xx)
                        def _():
                            near(zz, xx).wait_send()
                    else:
                        near(zz, xx).wait_send()

        @pl.when(relay)
        def _():
            for i in range(len(column)):
                forward(i).wait_send()


def shards(query_rows, cache_keys, cache_values, page_table, seq_lengths):
    slots, kv, page, dim = cache_keys.shape
    batch, heads, _ = query_rows.shape
    rows = heads // kv * batch
    devices = NX * NZ
    dma = pltpu.SemaphoreType.DMA
    return pl.pallas_call(
        kernel,
        out_shape=jax.ShapeDtypeStruct(query_rows.shape, query_rows.dtype),
        in_specs=[pl.BlockSpec(memory_space=pltpu.HBM)] * 5,
        out_specs=pl.BlockSpec(memory_space=pltpu.VMEM),
        scratch_shapes=[
            pltpu.SMEM(seq_lengths.shape, seq_lengths.dtype),
            pltpu.VMEM(query_rows.shape, query_rows.dtype),
            pltpu.VMEM((batch * heads, dim), jnp.float32),
            pltpu.VMEM((kv, slots, page, dim), cache_keys.dtype),
            pltpu.VMEM((kv, slots, page, dim), cache_values.dtype),
            pltpu.VMEM((page_table.shape[0] // page, page), jnp.int32),
            pltpu.VMEM((slots, batch, page), jnp.float32),
            pltpu.VMEM((kv // 2, 2 * rows, slots * page), jnp.float32),
            pltpu.VMEM((kv // 2, 2 * rows, slots * page), jnp.bfloat16),
            pltpu.VMEM((kv, rows, dim), jnp.int16),
            pltpu.VMEM((kv, 1, dim), jnp.float32),
            pltpu.VMEM((devices, rows, dim), jnp.int16),
            pltpu.VMEM((devices, 1, dim), jnp.float32),
            pltpu.VMEM((rows, dim), jnp.float32),
            pltpu.VMEM((1, dim), jnp.float32),
            pltpu.VMEM((1, dim), jnp.float32),
            pltpu.VMEM((kv, rows, dim), query_rows.dtype),
            pltpu.VMEM((heads * batch, dim), jnp.float32),
            dma((3,)),
            dma((kv,)),
            dma((kv,)),
            dma((kv,)),
            dma((kv,)),
            dma((devices,)),
            dma((devices,)),
            dma((NX * (NEAR + 2),)),
            dma((kv,)),
            dma((NZ - NEAR - 2,)),
            dma(()),
            pltpu.SemaphoreType.REGULAR,
        ],
        compiler_params=pltpu.CompilerParams(
            collective_id=0, has_side_effects=True, vmem_limit_bytes=40 << 20
        ),
        name="attend",
    )(
        *(
            pltpu.with_memory_space_constraint(a, pltpu.HBM)
            for a in (query_rows, cache_keys, cache_values, page_table.reshape(-1, page), seq_lengths)
        )
    )


def solution(mesh):
    return jax.shard_map(
        shards,
        mesh=mesh,
        in_specs=(
            P("grp", "head", None),
            P(("grp", "seq"), "head", None, None),
            P(("grp", "seq"), "head", None, None),
            P("grp"),
            P("grp"),
        ),
        out_specs=P("grp", "head", None),
        check_vma=False,
    )
```

```python
import functools
import math

import jax
import jax.numpy as jnp
from jax import lax
from jax.experimental import pallas as pl
from jax.experimental.pallas import tpu as pltpu
from jax.sharding import PartitionSpec as P

MESH = pl.DeviceIdType.MESH
NX, NZ = 4, 16
OWNER = 1
NEAR = 3
RELAY = 5
LATE = 13
VERY_LOW = -1e30
LEVELS = 32767.0


def remote(src, dst, send, recv, seq):
    return pltpu.make_async_remote_copy(
        src_ref=src,
        dst_ref=dst,
        send_sem=send,
        recv_sem=recv,
        device_id={"seq": seq},
        device_id_type=MESH,
    )


def diagonal(rows, lanes, first):
    lane = lax.broadcasted_iota(jnp.int32, (rows, lanes), 1)
    sub = lax.broadcasted_iota(jnp.int32, (rows, lanes), 0)
    return lane == sub + first


def to_column(row, rows):
    return jnp.sum(jnp.where(diagonal(rows, row.shape[1], 0), row, 0.0), axis=1, keepdims=True)


def kernel(
    q_hbm, k_hbm, v_hbm, table_hbm, len_hbm, out_ref,
    len_buf, q_buf, q_f32, k_buf0, k_buf1, v_buf0, v_buf1, table_buf, bias, scores0, scores1, probs0, probs1,
    numer16, stats, recv16, recv_stats, total_numer, total_row, top_row, finished, fin_f32,
    load_sem, k_sem, v_sem, send_p, recv_p, send_f, recv_f, send_w, ready,
):
    slots, kv, page, dim = k_hbm.shape
    batch, heads, _ = q_hbm.shape
    group = heads // kv
    table_rows = table_hbm.shape[0] // batch
    rows = group * batch
    pairs = [(g, g + 1) for g in range(0, kv, 2)]
    devices = NX * NZ

    load_t = pltpu.make_async_copy(table_hbm, table_buf, load_sem.at[0])
    load_l = pltpu.make_async_copy(len_hbm, len_buf, load_sem.at[1])
    load_q = pltpu.make_async_copy(q_hbm, q_buf, load_sem.at[2])
    k_buf, v_buf, scores, probs = (k_buf0, k_buf1), (v_buf0, v_buf1), (scores0, scores1), (probs0, probs1)
    loads_k = [
        pltpu.make_async_copy(k_hbm.at[:, pl.ds(2 * p, 2)], k_buf[p], k_sem.at[p]) for p in range(2)
    ]
    loads_v = [
        pltpu.make_async_copy(v_hbm.at[:, pl.ds(2 * p, 2)], v_buf[p], v_sem.at[p]) for p in range(2)
    ]
    load_t.start()
    load_l.start()
    load_q.start()
    loads_k[0].start()

    me = lax.axis_index("seq")
    x, z = me // NZ, me % NZ
    owner = z == OWNER
    relay = z == RELAY
    fed = jnp.logical_and(z > NEAR, jnp.logical_not(relay))
    owners = [g * NZ + OWNER for g in range(kv)]
    column = [zz for zz in range(NEAR + 1, NZ) if zz != RELAY]

    barrier = pltpu.get_barrier_semaphore()

    def signal(sem, other):
        pl.semaphore_signal(sem, inc=1, device_id={"seq": other}, device_id_type=MESH)

    @pl.when(owner)
    def _():
        @pl.loop(1, devices)
        def _(i):
            signal(barrier, (me + i) % devices)

    @pl.when(jnp.logical_not(owner))
    def _():
        for other in owners:
            signal(barrier, other)

    @pl.when(relay)
    def _():
        for zz in column:
            signal(barrier, x * NZ + zz)

    with jax.named_scope("tw"):
        load_t.wait()
        load_l.wait()
        load_q.wait()
    loads_k[1].start()
    loads_v[0].start()
    loads_v[1].start()
    first = me * slots
    lane = lax.broadcasted_iota(jnp.int32, (batch, page), 1)
    sub = lax.broadcasted_iota(jnp.int32, (batch, page), 0)
    length = jnp.zeros((batch, page), jnp.int32)
    for b in range(batch):
        length = jnp.where(sub == b, len_buf[b], length)
    tables = [table_buf[pl.ds(r, batch, stride=table_rows), :] for r in range(table_rows)]
    spans = [(length - page * (lane + page * r)).astype(jnp.float32) for r in range(table_rows)]
    lane_f32 = lane.astype(jnp.float32)
    for s in range(slots):
        found = functools.reduce(
            jnp.add, [jnp.where(t == first + s, n, 0.0) for t, n in zip(tables, spans)]
        )
        live = jnp.sum(found, axis=1, keepdims=True)
        bias[s] = jnp.where(lane_f32 < live, 0.0, VERY_LOW)
    q_f32[...] = q_buf[...].astype(jnp.float32).reshape(batch * heads, dim)

    factor = math.log2(math.e) / math.sqrt(dim)

    def sends(g):
        slot = z * NX + x
        return (
            remote(numer16.at[g], recv16.at[slot], send_p, recv_p.at[z], owners[g]),
            remote(stats.at[g], recv_stats.at[slot], send_p, recv_p.at[z], owners[g]),
        )

    def wait_for(sem, chunks):
        part = recv_stats.at[pl.ds(0, chunks * (rows // 2 + 1))]
        pltpu.make_async_copy(part, part, sem).wait()

    def wait_rows(sem, chunks):
        part = recv16.at[pl.ds(0, chunks)]
        pltpu.make_async_copy(part, part, sem).wait()

    def queries(p):
        blocks = []
        for i, g in enumerate(pairs[p]):
            query = jnp.concatenate(
                [q_f32[pl.ds(group * g + j, batch, stride=heads), :] for j in range(group)], axis=0
            ).astype(jnp.bfloat16)
            empty = jnp.zeros_like(query)
            blocks.append(jnp.concatenate([empty] * i + [query] + [empty] * (1 - i), axis=1))
        return jnp.concatenate(blocks, axis=0)

    def both(buf, s):
        return jnp.concatenate([buf[s : s + 2, i].reshape(2 * page, dim) for i in range(2)], axis=1)

    def score(p, query, s, best):
        got = lax.dot_general(
            query, both(k_buf[p], s), (((1,), (1,)), ((), ())), preferred_element_type=jnp.float32
        )
        for u in range(2):
            add = jnp.concatenate([bias[s + u]] * (2 * group), axis=0)
            now = got[:, u * page : (u + 1) * page] * factor + add
            scores[p][:, (s + u) * page : (s + u + 1) * page] = now
            best = now if best is None else jnp.maximum(best, now)
        return best

    def weigh(p, top, s, total):
        for u in range(s, s + 2):
            w = jnp.exp2(scores[p][:, u * page : (u + 1) * page] - top)
            total = w if total is None else total + w
            probs[p][:, u * page : (u + 1) * page] = w.astype(jnp.bfloat16)
        return total

    def attend(p, s, numers):
        now = jnp.dot(
            probs[p][:, s * page : (s + 2) * page], both(v_buf[p], s), preferred_element_type=jnp.float32
        )
        return now if numers is None else numers + now

    def finish(p, numers, top, total):
        total = jnp.sum(total, axis=1, keepdims=True)
        for i, g in enumerate(pairs[p]):
            own = slice(i * rows, (i + 1) * rows)
            numer = numers[own, i * dim : (i + 1) * dim]
            largest = jnp.max(jnp.abs(numer), axis=1, keepdims=True)
            steps = numer * (LEVELS / jnp.maximum(largest, 1e-30))
            numer16[g] = jnp.floor(steps + 0.5).astype(jnp.int32).astype(jnp.int16)
            row = sum(
                jnp.where(diagonal(rows, dim, j * rows), c, 0.0)
                for j, c in enumerate((top[own], total[own], largest * (1.0 / LEVELS)))
            )
            stats[g] = jnp.sum(row, axis=0, keepdims=True)

        @pl.when(jnp.logical_not(owner))
        def _():
            with jax.named_scope(f"snd{p}"):
                for g in pairs[p]:
                    for c in sends(g):
                        c.start()

    steps = range(0, slots, 2)
    query0, query1 = queries(0), queries(1)
    with jax.named_scope("kw0"):
        loads_k[0].wait()
    best0 = None
    for s in steps:
        best0 = score(0, query0, s, best0)
    top0 = jnp.max(best0, axis=1, keepdims=True)
    with jax.named_scope("kw1"):
        loads_k[1].wait()
    best1, total0 = None, None
    for s in steps:
        best1 = score(1, query1, s, best1)
        total0 = weigh(0, top0, s, total0)
    top1 = jnp.max(best1, axis=1, keepdims=True)

    with jax.named_scope("bw"):

        @pl.when(fed)
        def _():
            pl.semaphore_wait(barrier, kv + 1)
            signal(ready, x * NZ + RELAY)

        @pl.when(jnp.logical_not(jnp.logical_or(owner, fed)))
        def _():
            pl.semaphore_wait(barrier, kv)

    with jax.named_scope("vw0"):
        loads_v[0].wait()
    numers0, total1 = None, None
    for s in steps:
        numers0 = attend(0, s, numers0)
        total1 = weigh(1, top1, s, total1)
    finish(0, numers0, top0, total0)
    with jax.named_scope("vw1"):
        loads_v[1].wait()
    numers1 = None
    for s in steps:
        numers1 = attend(1, s, numers1)
    finish(1, numers1, top1, total1)

    def near(zz, xx):
        other = xx * NZ + zz
        return remote(
            finished.at[x], finished.at[x], send_f, recv_f, other
        )

    near_z = [*range(NEAR + 1), RELAY]

    @pl.when(owner)
    def _():
        with jax.named_scope("bar"):
            pl.semaphore_wait(barrier, devices - 1)
        for g in range(kv):

            @pl.when(x != g)
            def _():
                for c in sends(g):
                    c.start()

        slot = z * NX + x
        recv16[slot] = numer16[x]
        recv_stats[slot] = stats[x]
        total_numer[...] = jnp.zeros_like(total_numer)
        total_row[...] = jnp.zeros_like(total_row)
        top_row[...] = jnp.full_like(top_row, VERY_LOW)

        def add(zz, chunks=NX):
            sources = [zz * NX + xx for xx in range(NX)]
            with jax.named_scope("rw"):
                wait_for(recv_p.at[zz], chunks)

            got = jnp.concatenate([recv_stats[src] for src in sources] * 2, axis=0)
            totals = pltpu.roll(got, dim - rows, 1)
            scales = pltpu.roll(got, dim - 2 * rows, 1)
            before = top_row[...]
            top = jnp.maximum(before, jnp.max(got, axis=0, keepdims=True))
            weight = jnp.exp2(got - top)
            keep = jnp.exp2(before - top)
            top_row[...] = top
            weighted = weight * totals
            new_total = total_row[...] * keep
            for i in range(NX):
                new_total = new_total + weighted[i : i + 1]
            total_row[...] = new_total
            scaled = weight * scales
            numer = total_numer[...] * to_column(keep, rows)
            for i, src in enumerate(sources):
                numer = numer + recv16[src].astype(jnp.int32).astype(jnp.float32) * to_column(
                    scaled[i : i + 1], rows
                )
            total_numer[...] = numer

        @pl.loop(OWNER + 1, LATE)
        def _(zz):
            add(zz)

        add(OWNER, NX - 1)
        add(0)

        @pl.loop(LATE, NZ)
        def _(zz):
            add(zz)

        done = total_numer[...] / to_column(total_row[...], rows)
        finished[x] = done.astype(finished.dtype)
        with jax.named_scope("bcast"):
            for zz in near_z:
                for xx in range(NX):
                    if zz == OWNER:

                        @pl.when(x != xx)
                        def _():
                            near(zz, xx).start()
                    else:
                        near(zz, xx).start()

    def forward(i):
        return remote(finished, finished, send_w, recv_f, x * NZ + column[i])

    with jax.named_scope("fw"):

        @pl.when(owner)
        def _():
            wait_rows(recv_f, kv - 1)

        @pl.when(jnp.logical_not(owner))
        def _():
            wait_rows(recv_f, kv)

    @pl.when(relay)
    def _():
        pl.semaphore_wait(ready, len(column))
        for i in range(len(column)):
            forward(i).start()

    fin_f32[...] = finished[...].astype(jnp.float32).reshape(heads * batch, dim)
    for b in range(batch):
        out_ref[b] = fin_f32[pl.ds(b, heads, stride=batch), :].astype(out_ref.dtype)

    with jax.named_scope("ws"):

        @pl.when(owner)
        def _():
            wait_for(send_p, kv - 1)
            wait_rows(send_f, len(near_z) * NX - 1)

        @pl.when(jnp.logical_not(owner))
        def _():
            wait_for(send_p, kv)

        @pl.when(relay)
        def _():
            wait_rows(send_w, len(column) * kv)


def shards(query_rows, cache_keys, cache_values, page_table, seq_lengths):
    slots, kv, page, dim = cache_keys.shape
    batch, heads, _ = query_rows.shape
    rows = heads // kv * batch
    devices = NX * NZ
    dma = pltpu.SemaphoreType.DMA
    return pl.pallas_call(
        kernel,
        out_shape=jax.ShapeDtypeStruct(query_rows.shape, query_rows.dtype),
        in_specs=[pl.BlockSpec(memory_space=pltpu.HBM)] * 5,
        out_specs=pl.BlockSpec(memory_space=pltpu.VMEM),
        scratch_shapes=[
            pltpu.SMEM(seq_lengths.shape, seq_lengths.dtype),
            pltpu.VMEM(query_rows.shape, query_rows.dtype),
            pltpu.VMEM((batch * heads, dim), jnp.float32),
            pltpu.VMEM((slots, 2, page, dim), cache_keys.dtype),
            pltpu.VMEM((slots, 2, page, dim), cache_keys.dtype),
            pltpu.VMEM((slots, 2, page, dim), cache_values.dtype),
            pltpu.VMEM((slots, 2, page, dim), cache_values.dtype),
            pltpu.VMEM((page_table.shape[0] // page, page), jnp.int32),
            pltpu.VMEM((slots, batch, page), jnp.float32),
            pltpu.VMEM((2 * rows, slots * page), jnp.float32),
            pltpu.VMEM((2 * rows, slots * page), jnp.float32),
            pltpu.VMEM((2 * rows, slots * page), jnp.bfloat16),
            pltpu.VMEM((2 * rows, slots * page), jnp.bfloat16),
            pltpu.VMEM((kv, rows, dim), jnp.int16),
            pltpu.VMEM((kv, 1, dim), jnp.float32),
            pltpu.VMEM((devices, rows, dim), jnp.int16),
            pltpu.VMEM((NX * (rows // 2 + 1), 1, dim), jnp.float32),
            pltpu.VMEM((rows, dim), jnp.float32),
            pltpu.VMEM((1, dim), jnp.float32),
            pltpu.VMEM((1, dim), jnp.float32),
            pltpu.VMEM((kv, rows, dim), query_rows.dtype),
            pltpu.VMEM((heads * batch, dim), jnp.float32),
            dma((3,)),
            dma((2,)),
            dma((2,)),
            dma(()),
            dma((NZ,)),
            dma(()),
            dma(()),
            dma(()),
            pltpu.SemaphoreType.REGULAR,
        ],
        compiler_params=pltpu.CompilerParams(
            collective_id=0, has_side_effects=True, vmem_limit_bytes=40 << 20
        ),
        name="attend",
    )(
        *(
            pltpu.with_memory_space_constraint(a, pltpu.HBM)
            for a in (query_rows, cache_keys, cache_values, page_table.reshape(-1, page), seq_lengths)
        )
    )


def solution(mesh):
    return jax.shard_map(
        shards,
        mesh=mesh,
        in_specs=(
            P("grp", "head", None),
            P(("grp", "seq"), "head", None, None),
            P(("grp", "seq"), "head", None, None),
            P("grp"),
            P("grp"),
        ),
        out_specs=P("grp", "head", None),
        check_vma=False,
    )
```

```python
import functools
import math

import jax
import jax.numpy as jnp
from jax import lax
from jax.experimental import pallas as pl
from jax.experimental.pallas import tpu as pltpu
from jax.sharding import PartitionSpec as P

MESH = pl.DeviceIdType.MESH
NX, NZ = 4, 16
OWNER = 1
NEAR = 3
RELAY = 5
LATE = 13
VERY_LOW = -1e30
LOWEST = -3e38
LEVELS = 32767.0


def remote(src, dst, send, recv, seq):
    return pltpu.make_async_remote_copy(
        src_ref=src,
        dst_ref=dst,
        send_sem=send,
        recv_sem=recv,
        device_id={"seq": seq},
        device_id_type=MESH,
    )


def diagonal(rows, lanes, first):
    lane = lax.broadcasted_iota(jnp.int32, (rows, lanes), 1)
    sub = lax.broadcasted_iota(jnp.int32, (rows, lanes), 0)
    return lane == sub + first


def to_column(row, rows):
    return jnp.sum(jnp.where(diagonal(rows, row.shape[1], 0), row, 0.0), axis=1, keepdims=True)


def kernel(
    q_hbm, k_hbm, v_hbm, table_hbm, len_hbm, out_ref,
    len_buf, q_buf, q_f32, k_buf0, k_buf1, v_buf0, v_buf1, table_buf, bias, scores0, scores1, probs0, probs1,
    numer16, stats, recv16, recv_stats, total_numer, total_row, top_row, finished, fin_f32,
    load_sem, k_sem, v_sem, send_p, recv_p, send_f, recv_f, send_w, ready,
):
    slots, kv, page, dim = k_hbm.shape
    batch, heads, _ = q_hbm.shape
    group = heads // kv
    table_rows = table_hbm.shape[0] // batch
    rows = group * batch
    pairs = [(g, g + 1) for g in range(0, kv, 2)]
    devices = NX * NZ

    load_t = pltpu.make_async_copy(table_hbm, table_buf, load_sem.at[0])
    load_l = pltpu.make_async_copy(len_hbm, len_buf, load_sem.at[1])
    load_q = pltpu.make_async_copy(q_hbm, q_buf, load_sem.at[2])
    k_buf, v_buf, scores, probs = (k_buf0, k_buf1), (v_buf0, v_buf1), (scores0, scores1), (probs0, probs1)
    half = slots // 2

    def loads(source, target, p, sems, parts):
        size = slots // parts
        return [
            pltpu.make_async_copy(
                source.at[pl.ds(i * size, size), pl.ds(2 * p, 2)], target.at[pl.ds(i * size, size)], sems.at[i]
            )
            for i in range(parts)
        ]

    loads_k0 = loads(k_hbm, k_buf0, 0, k_sem.at[pl.ds(0, 2)], 2)
    loads_k1 = loads(k_hbm, k_buf1, 1, k_sem.at[pl.ds(2, 1)], 1)
    loads_v0 = loads(v_hbm, v_buf0, 0, v_sem.at[pl.ds(0, 1)], 1)
    loads_v1 = loads(v_hbm, v_buf1, 1, v_sem.at[pl.ds(1, 2)], 2)

    load_t.start()
    load_l.start()
    load_q.start()
    for c in loads_k0:
        c.start()

    me = lax.axis_index("seq")
    x, z = me // NZ, me % NZ
    owner = z == OWNER
    relay = z == RELAY
    fed = jnp.logical_and(z > NEAR, jnp.logical_not(relay))
    owners = [g * NZ + OWNER for g in range(kv)]
    column = [zz for zz in range(NEAR + 1, NZ) if zz != RELAY]

    barrier = pltpu.get_barrier_semaphore()

    def signal(sem, other):
        pl.semaphore_signal(sem, inc=1, device_id={"seq": other}, device_id_type=MESH)

    @pl.when(owner)
    def _():
        @pl.loop(1, devices)
        def _(i):
            signal(barrier, (me + i) % devices)

    @pl.when(jnp.logical_not(owner))
    def _():
        for other in owners:
            signal(barrier, other)

    @pl.when(relay)
    def _():
        for zz in column:
            signal(barrier, x * NZ + zz)

    with jax.named_scope("tw"):
        load_t.wait()
        load_l.wait()
        load_q.wait()
    loads_v0[0].start()
    first = me * slots
    lane = lax.broadcasted_iota(jnp.int32, (batch, page), 1)
    sub = lax.broadcasted_iota(jnp.int32, (batch, page), 0)
    length = jnp.zeros((batch, page), jnp.int32)
    for b in range(batch):
        length = jnp.where(sub == b, len_buf[b], length)
    tables = [table_buf[pl.ds(r, batch, stride=table_rows), :] for r in range(table_rows)]
    spans = [(length - page * (lane + page * r)).astype(jnp.float32) for r in range(table_rows)]
    lane_f32 = lane.astype(jnp.float32)
    for s in range(slots):
        found = functools.reduce(
            jnp.add, [jnp.where(t == first + s, n, 0.0) for t, n in zip(tables, spans)]
        )
        live = jnp.sum(found, axis=1, keepdims=True)
        bias[s] = jnp.where(lane_f32 < live, 0.0, VERY_LOW)
    q_f32[...] = q_buf[...].astype(jnp.float32).reshape(batch * heads, dim)

    factor = math.log2(math.e) / math.sqrt(dim)

    def sends(g):
        slot = z * NX + x
        return (
            remote(numer16.at[g], recv16.at[slot], send_p, recv_p.at[z], owners[g]),
            remote(stats.at[g], recv_stats.at[slot], send_p, recv_p.at[z], owners[g]),
        )

    def wait_for(sem, chunks):
        part = recv_stats.at[pl.ds(0, chunks * (rows // 2 + 1))]
        pltpu.make_async_copy(part, part, sem).wait()

    def wait_rows(sem, chunks):
        part = recv16.at[pl.ds(0, chunks)]
        pltpu.make_async_copy(part, part, sem).wait()

    def queries(p):
        blocks = []
        for i, g in enumerate(pairs[p]):
            query = jnp.concatenate(
                [q_f32[pl.ds(group * g + j, batch, stride=heads), :] for j in range(group)], axis=0
            ).astype(jnp.bfloat16)
            empty = jnp.zeros_like(query)
            blocks.append(jnp.concatenate([empty] * i + [query] + [empty] * (1 - i), axis=1))
        return jnp.concatenate(blocks, axis=0)

    def both(buf, s):
        return jnp.concatenate([buf[s : s + 2, i].reshape(2 * page, dim) for i in range(2)], axis=1)

    def score(p, query, s, best):
        got = lax.dot_general(
            query, both(k_buf[p], s), (((1,), (1,)), ((), ())), preferred_element_type=jnp.float32
        )
        for u in range(2):
            add = jnp.concatenate([bias[s + u]] * (2 * group), axis=0)
            now = got[:, u * page : (u + 1) * page] * factor + add
            scores[p][:, (s + u) * page : (s + u + 1) * page] = now
            best = now if best is None else jnp.maximum(best, now)
        return best

    def weigh(p, top, s, total):
        for u in range(s, s + 2):
            w = jnp.exp2(scores[p][:, u * page : (u + 1) * page] - top)
            total = w if total is None else total + w
            probs[p][:, u * page : (u + 1) * page] = w.astype(jnp.bfloat16)
        return total

    def attend(p, s, numers):
        now = jnp.dot(
            probs[p][:, s * page : (s + 2) * page], both(v_buf[p], s), preferred_element_type=jnp.float32
        )
        turn = s // 2 % 2
        numers[turn] = now if numers[turn] is None else numers[turn] + now

    def joined(sums):
        return jnp.maximum(sums[0], LOWEST) + sums[1]

    def finish(p, numers, top, total):
        total = jnp.sum(total, axis=1, keepdims=True)
        for i, g in enumerate(pairs[p]):
            own = slice(i * rows, (i + 1) * rows)
            numer = numers[own, i * dim : (i + 1) * dim]
            largest = jnp.max(jnp.abs(numer), axis=1, keepdims=True)
            steps = numer * (LEVELS / jnp.maximum(largest, 1e-30))
            numer16[g] = jnp.floor(steps + 0.5).astype(jnp.int32).astype(jnp.int16)
            row = sum(
                jnp.where(diagonal(rows, dim, j * rows), c, 0.0)
                for j, c in enumerate((top[own], total[own], largest * (1.0 / LEVELS)))
            )
            stats[g] = jnp.sum(row, axis=0, keepdims=True)

        @pl.when(jnp.logical_not(owner))
        def _():
            with jax.named_scope(f"snd{p}"):
                for g in pairs[p]:
                    for c in sends(g):
                        c.start()

    steps = range(0, slots, 2)
    query0, query1 = queries(0), queries(1)
    best0 = None
    for i in range(2):
        with jax.named_scope(f"kw0{i}"):
            loads_k0[i].wait()
        if i == 1:
            loads_k1[0].start()
        for s in range(i * half, (i + 1) * half, 2):
            best0 = score(0, query0, s, best0)
    top0 = jnp.max(best0, axis=1, keepdims=True)
    with jax.named_scope("vw0"):
        loads_v0[0].wait()
    for c in loads_v1:
        c.start()
    numers0, total0 = [None, None], None
    for s in steps:
        total0 = weigh(0, top0, s, total0)
        attend(0, s, numers0)

    with jax.named_scope("bw"):

        @pl.when(fed)
        def _():
            pl.semaphore_wait(barrier, kv + 1)
            signal(ready, x * NZ + RELAY)

        @pl.when(jnp.logical_not(jnp.logical_or(owner, fed)))
        def _():
            pl.semaphore_wait(barrier, kv)

    finish(0, joined(numers0), top0, total0)
    with jax.named_scope("kw1"):
        loads_k1[0].wait()
    best1 = None
    for s in steps:
        best1 = score(1, query1, s, best1)
    top1 = jnp.max(best1, axis=1, keepdims=True)
    numers1, total1 = [None, None], None
    for i in range(2):
        with jax.named_scope(f"vw1{i}"):
            loads_v1[i].wait()
        for s in range(i * half, (i + 1) * half, 2):
            total1 = weigh(1, top1, s, total1)
            attend(1, s, numers1)
    finish(1, joined(numers1), top1, total1)

    def near(zz, xx):
        other = xx * NZ + zz
        return remote(
            finished.at[x], finished.at[x], send_f, recv_f, other
        )

    near_z = [*range(NEAR + 1), RELAY]

    @pl.when(owner)
    def _():
        with jax.named_scope("bar"):
            pl.semaphore_wait(barrier, devices - 1)
        for g in range(kv):

            @pl.when(x != g)
            def _():
                for c in sends(g):
                    c.start()

        slot = z * NX + x
        recv16[slot] = numer16[x]
        recv_stats[slot] = stats[x]
        total_numer[...] = jnp.zeros_like(total_numer)
        total_row[...] = jnp.zeros_like(total_row)
        top_row[...] = jnp.full_like(top_row, VERY_LOW)

        def add(zz, chunks=NX):
            sources = [zz * NX + xx for xx in range(NX)]
            with jax.named_scope("rw"):
                wait_for(recv_p.at[zz], chunks)

            got = jnp.concatenate([recv_stats[src] for src in sources] * 2, axis=0)
            totals = pltpu.roll(got, dim - rows, 1)
            scales = pltpu.roll(got, dim - 2 * rows, 1)
            before = top_row[...]
            top = jnp.maximum(before, jnp.max(got, axis=0, keepdims=True))
            weight = jnp.exp2(got - top)
            keep = jnp.exp2(before - top)
            top_row[...] = top
            weighted = weight * totals
            new_total = total_row[...] * keep
            for i in range(NX):
                new_total = new_total + weighted[i : i + 1]
            total_row[...] = new_total
            scaled = weight * scales
            numer = total_numer[...] * to_column(keep, rows)
            for i, src in enumerate(sources):
                numer = numer + recv16[src].astype(jnp.int32).astype(jnp.float32) * to_column(
                    scaled[i : i + 1], rows
                )
            total_numer[...] = numer

        @pl.loop(OWNER + 1, LATE)
        def _(zz):
            add(zz)

        add(OWNER, NX - 1)
        add(0)

        @pl.loop(LATE, NZ)
        def _(zz):
            add(zz)

        done = total_numer[...] / to_column(total_row[...], rows)
        finished[x] = done.astype(finished.dtype)
        with jax.named_scope("bcast"):
            for zz in near_z:
                for xx in range(NX):
                    if zz == OWNER:

                        @pl.when(x != xx)
                        def _():
                            near(zz, xx).start()
                    else:
                        near(zz, xx).start()

    def forward(i):
        return remote(finished, finished, send_w, recv_f, x * NZ + column[i])

    with jax.named_scope("fw"):

        @pl.when(owner)
        def _():
            wait_rows(recv_f, kv - 1)

        @pl.when(jnp.logical_not(owner))
        def _():
            wait_rows(recv_f, kv)

    @pl.when(relay)
    def _():
        pl.semaphore_wait(ready, len(column))
        for i in range(len(column)):
            forward(i).start()

    fin_f32[...] = finished[...].astype(jnp.float32).reshape(heads * batch, dim)
    for b in range(batch):
        out_ref[b] = fin_f32[pl.ds(b, heads, stride=batch), :].astype(out_ref.dtype)

    with jax.named_scope("ws"):

        @pl.when(owner)
        def _():
            wait_for(send_p, kv - 1)
            wait_rows(send_f, len(near_z) * NX - 1)

        @pl.when(jnp.logical_not(owner))
        def _():
            wait_for(send_p, kv)

        @pl.when(relay)
        def _():
            wait_rows(send_w, len(column) * kv)


def shards(query_rows, cache_keys, cache_values, page_table, seq_lengths):
    slots, kv, page, dim = cache_keys.shape
    batch, heads, _ = query_rows.shape
    rows = heads // kv * batch
    devices = NX * NZ
    dma = pltpu.SemaphoreType.DMA
    return pl.pallas_call(
        kernel,
        out_shape=jax.ShapeDtypeStruct(query_rows.shape, query_rows.dtype),
        in_specs=[pl.BlockSpec(memory_space=pltpu.HBM)] * 5,
        out_specs=pl.BlockSpec(memory_space=pltpu.VMEM),
        scratch_shapes=[
            pltpu.SMEM(seq_lengths.shape, seq_lengths.dtype),
            pltpu.VMEM(query_rows.shape, query_rows.dtype),
            pltpu.VMEM((batch * heads, dim), jnp.float32),
            pltpu.VMEM((slots, 2, page, dim), cache_keys.dtype),
            pltpu.VMEM((slots, 2, page, dim), cache_keys.dtype),
            pltpu.VMEM((slots, 2, page, dim), cache_values.dtype),
            pltpu.VMEM((slots, 2, page, dim), cache_values.dtype),
            pltpu.VMEM((page_table.shape[0] // page, page), jnp.int32),
            pltpu.VMEM((slots, batch, page), jnp.float32),
            pltpu.VMEM((2 * rows, slots * page), jnp.float32),
            pltpu.VMEM((2 * rows, slots * page), jnp.float32),
            pltpu.VMEM((2 * rows, slots * page), jnp.bfloat16),
            pltpu.VMEM((2 * rows, slots * page), jnp.bfloat16),
            pltpu.VMEM((kv, rows, dim), jnp.int16),
            pltpu.VMEM((kv, 1, dim), jnp.float32),
            pltpu.VMEM((devices, rows, dim), jnp.int16),
            pltpu.VMEM((NX * (rows // 2 + 1), 1, dim), jnp.float32),
            pltpu.VMEM((rows, dim), jnp.float32),
            pltpu.VMEM((1, dim), jnp.float32),
            pltpu.VMEM((1, dim), jnp.float32),
            pltpu.VMEM((kv, rows, dim), query_rows.dtype),
            pltpu.VMEM((heads * batch, dim), jnp.float32),
            dma((3,)),
            dma((3,)),
            dma((3,)),
            dma(()),
            dma((NZ,)),
            dma(()),
            dma(()),
            dma(()),
            pltpu.SemaphoreType.REGULAR,
        ],
        compiler_params=pltpu.CompilerParams(
            collective_id=0, has_side_effects=True, vmem_limit_bytes=40 << 20
        ),
        name="attend",
    )(
        *(
            pltpu.with_memory_space_constraint(a, pltpu.HBM)
            for a in (query_rows, cache_keys, cache_values, page_table.reshape(-1, page), seq_lengths)
        )
    )


def solution(mesh):
    return jax.shard_map(
        shards,
        mesh=mesh,
        in_specs=(
            P("grp", "head", None),
            P(("grp", "seq"), "head", None, None),
            P(("grp", "seq"), "head", None, None),
            P("grp"),
            P("grp"),
        ),
        out_specs=P("grp", "head", None),
        check_vma=False,
    )
```

```python
import functools
import math

import jax
import jax.numpy as jnp
from jax import lax
from jax.experimental import pallas as pl
from jax.experimental.pallas import tpu as pltpu
from jax.sharding import PartitionSpec as P

MESH = pl.DeviceIdType.MESH
NX, NZ = 4, 16
OWNER = 1
NEAR = 3
RELAY = 5
LATE = 13
VERY_LOW = -1e30
LOWEST = -3e38
LEVELS = 32767.0


def remote(src, dst, send, recv, seq):
    return pltpu.make_async_remote_copy(
        src_ref=src,
        dst_ref=dst,
        send_sem=send,
        recv_sem=recv,
        device_id={"seq": seq},
        device_id_type=MESH,
    )


def diagonal(rows, lanes, first):
    lane = lax.broadcasted_iota(jnp.int32, (rows, lanes), 1)
    sub = lax.broadcasted_iota(jnp.int32, (rows, lanes), 0)
    return lane == sub + first


def to_column(row, rows):
    return jnp.sum(jnp.where(diagonal(rows, row.shape[1], 0), row, 0.0), axis=1, keepdims=True)


def kernel(
    q_hbm, k_hbm, v_hbm, table_hbm, len_hbm, out_ref,
    len_buf, q_buf, q_f32, k_buf0, k_buf1, v_buf0, v_buf1, table_buf, bias, scores0, scores1, probs0, probs1,
    numer16, stats, recv16, recv_stats, total_numer, total_row, top_row, finished, fin_f32,
    load_sem, k_sem, v_sem, send_p, recv_p, send_f, recv_f, send_w, ready,
):
    slots, kv, page, dim = k_hbm.shape
    batch, heads, _ = q_hbm.shape
    group = heads // kv
    table_rows = table_hbm.shape[0] // batch
    rows = group * batch
    pairs = [(g, g + 1) for g in range(0, kv, 2)]
    devices = NX * NZ

    load_t = pltpu.make_async_copy(table_hbm, table_buf, load_sem.at[0])
    load_l = pltpu.make_async_copy(len_hbm, len_buf, load_sem.at[1])
    load_q = pltpu.make_async_copy(q_hbm, q_buf, load_sem.at[2])
    k_buf, v_buf, scores, probs = (k_buf0, k_buf1), (v_buf0, v_buf1), (scores0, scores1), (probs0, probs1)
    half = slots // 2

    def loads(source, target, p, sems, parts):
        size = slots // parts
        return [
            pltpu.make_async_copy(
                source.at[pl.ds(i * size, size), pl.ds(2 * p, 2)], target.at[pl.ds(i * size, size)], sems.at[i]
            )
            for i in range(parts)
        ]

    loads_k0 = loads(k_hbm, k_buf0, 0, k_sem.at[pl.ds(0, 2)], 2)
    loads_k1 = loads(k_hbm, k_buf1, 1, k_sem.at[pl.ds(2, 1)], 1)
    loads_v0 = loads(v_hbm, v_buf0, 0, v_sem.at[pl.ds(0, 1)], 1)
    loads_v1 = loads(v_hbm, v_buf1, 1, v_sem.at[pl.ds(1, 2)], 2)

    load_t.start()
    load_l.start()
    load_q.start()
    loads_k0[0].start()
    loads_k0[1].start()
    loads_v0[0].start()

    me = lax.axis_index("seq")
    x, z = me // NZ, me % NZ
    owner = z == OWNER
    relay = z == RELAY
    fed = jnp.logical_and(z > NEAR, jnp.logical_not(relay))
    owners = [g * NZ + OWNER for g in range(kv)]
    column = [zz for zz in range(NEAR + 1, NZ) if zz != RELAY]

    barrier = pltpu.get_barrier_semaphore()

    def signal(sem, other):
        pl.semaphore_signal(sem, inc=1, device_id={"seq": other}, device_id_type=MESH)

    @pl.when(owner)
    def _():
        @pl.loop(1, devices)
        def _(i):
            signal(barrier, (me + i) % devices)

    @pl.when(jnp.logical_not(owner))
    def _():
        for other in owners:
            signal(barrier, other)

    @pl.when(relay)
    def _():
        for zz in column:
            signal(barrier, x * NZ + zz)

    with jax.named_scope("tw"):
        load_t.wait()
        load_l.wait()
        load_q.wait()
    loads_k1[0].start()
    first = me * slots
    lane = lax.broadcasted_iota(jnp.int32, (batch, page), 1)
    sub = lax.broadcasted_iota(jnp.int32, (batch, page), 0)
    length = jnp.zeros((batch, page), jnp.int32)
    for b in range(batch):
        length = jnp.where(sub == b, len_buf[b], length)
    tables = [table_buf[pl.ds(r, batch, stride=table_rows), :] for r in range(table_rows)]
    spans = [(length - page * (lane + page * r)).astype(jnp.float32) for r in range(table_rows)]
    lane_f32 = lane.astype(jnp.float32)
    for s in range(slots):
        found = functools.reduce(
            jnp.add, [jnp.where(t == first + s, n, 0.0) for t, n in zip(tables, spans)]
        )
        live = jnp.sum(found, axis=1, keepdims=True)
        bias[s] = jnp.where(lane_f32 < live, 0.0, VERY_LOW)
    q_f32[...] = q_buf[...].astype(jnp.float32).reshape(batch * heads, dim)

    factor = math.log2(math.e) / math.sqrt(dim)

    def sends(g):
        slot = z * NX + x
        return (
            remote(numer16.at[g], recv16.at[slot], send_p, recv_p.at[z], owners[g]),
            remote(stats.at[g], recv_stats.at[slot], send_p, recv_p.at[z], owners[g]),
        )

    def wait_for(sem, chunks):
        part = recv_stats.at[pl.ds(0, chunks * (rows // 2 + 1))]
        pltpu.make_async_copy(part, part, sem).wait()

    def wait_rows(sem, chunks):
        part = recv16.at[pl.ds(0, chunks)]
        pltpu.make_async_copy(part, part, sem).wait()

    def queries(p):
        blocks = []
        for i, g in enumerate(pairs[p]):
            query = jnp.concatenate(
                [q_f32[pl.ds(group * g + j, batch, stride=heads), :] for j in range(group)], axis=0
            ).astype(jnp.bfloat16)
            empty = jnp.zeros_like(query)
            blocks.append(jnp.concatenate([empty] * i + [query] + [empty] * (1 - i), axis=1))
        return jnp.concatenate(blocks, axis=0)

    def both(buf, s):
        return jnp.concatenate([buf[s : s + 2, i].reshape(2 * page, dim) for i in range(2)], axis=1)

    def score(p, query, s, best):
        got = lax.dot_general(
            query, both(k_buf[p], s), (((1,), (1,)), ((), ())), preferred_element_type=jnp.float32
        )
        for u in range(2):
            add = jnp.concatenate([bias[s + u]] * (2 * group), axis=0)
            now = got[:, u * page : (u + 1) * page] * factor + add
            scores[p][:, (s + u) * page : (s + u + 1) * page] = now
            best = now if best is None else jnp.maximum(best, now)
        return best

    def weigh(p, top, s, total):
        for u in range(s, s + 2):
            w = jnp.exp2(scores[p][:, u * page : (u + 1) * page] - top)
            total = w if total is None else total + w
            probs[p][:, u * page : (u + 1) * page] = w.astype(jnp.bfloat16)
        return total

    def attend(p, s, numers):
        now = jnp.dot(
            probs[p][:, s * page : (s + 2) * page], both(v_buf[p], s), preferred_element_type=jnp.float32
        )
        turn = s // 2 % 2
        numers[turn] = now if numers[turn] is None else numers[turn] + now

    def joined(sums):
        return jnp.maximum(sums[0], LOWEST) + sums[1]

    def finish(p, numers, top, total):
        total = jnp.sum(total, axis=1, keepdims=True)
        for i, g in enumerate(pairs[p]):
            own = slice(i * rows, (i + 1) * rows)
            numer = numers[own, i * dim : (i + 1) * dim]
            largest = jnp.max(jnp.abs(numer), axis=1, keepdims=True)
            steps = numer * (LEVELS / jnp.maximum(largest, 1e-30))
            numer16[g] = jnp.floor(steps + 0.5).astype(jnp.int32).astype(jnp.int16)
            row = sum(
                jnp.where(diagonal(rows, dim, j * rows), c, 0.0)
                for j, c in enumerate((top[own], total[own], largest * (1.0 / LEVELS)))
            )
            stats[g] = jnp.sum(row, axis=0, keepdims=True)

        @pl.when(jnp.logical_not(owner))
        def _():
            with jax.named_scope(f"snd{p}"):
                for g in pairs[p]:
                    for c in sends(g):
                        c.start()

    steps = range(0, slots, 2)
    query0, query1 = queries(0), queries(1)
    best0 = None
    for i in range(2):
        with jax.named_scope(f"kw0{i}"):
            loads_k0[i].wait()
        if i == 0:
            loads_v1[0].start()
            loads_v1[1].start()
        for s in range(i * half, (i + 1) * half, 2):
            best0 = score(0, query0, s, best0)
    top0 = jnp.max(best0, axis=1, keepdims=True)
    with jax.named_scope("vw0"):
        loads_v0[0].wait()
    numers0, total0 = [None, None], None
    for s in steps:
        total0 = weigh(0, top0, s, total0)
        attend(0, s, numers0)

    with jax.named_scope("bw"):

        @pl.when(fed)
        def _():
            pl.semaphore_wait(barrier, kv + 1)
            signal(ready, x * NZ + RELAY)

        @pl.when(jnp.logical_not(jnp.logical_or(owner, fed)))
        def _():
            pl.semaphore_wait(barrier, kv)

    finish(0, joined(numers0), top0, total0)
    with jax.named_scope("kw1"):
        loads_k1[0].wait()
    best1 = None
    for s in steps:
        best1 = score(1, query1, s, best1)
    top1 = jnp.max(best1, axis=1, keepdims=True)
    numers1, total1 = [None, None], None
    for i in range(2):
        with jax.named_scope(f"vw1{i}"):
            loads_v1[i].wait()
        for s in range(i * half, (i + 1) * half, 2):
            total1 = weigh(1, top1, s, total1)
            attend(1, s, numers1)
    finish(1, joined(numers1), top1, total1)

    def near(zz, xx):
        other = xx * NZ + zz
        return remote(
            finished.at[x], finished.at[x], send_f, recv_f, other
        )

    near_z = [*range(NEAR + 1), RELAY]

    @pl.when(owner)
    def _():
        with jax.named_scope("bar"):
            pl.semaphore_wait(barrier, devices - 1)
        for g in range(kv):

            @pl.when(x != g)
            def _():
                for c in sends(g):
                    c.start()

        slot = z * NX + x
        recv16[slot] = numer16[x]
        recv_stats[slot] = stats[x]
        total_numer[...] = jnp.zeros_like(total_numer)
        total_row[...] = jnp.zeros_like(total_row)
        top_row[...] = jnp.full_like(top_row, VERY_LOW)

        def add(zz, chunks=NX):
            sources = [zz * NX + xx for xx in range(NX)]
            with jax.named_scope("rw"):
                wait_for(recv_p.at[zz], chunks)

            got = jnp.concatenate([recv_stats[src] for src in sources] * 2, axis=0)
            totals = pltpu.roll(got, dim - rows, 1)
            scales = pltpu.roll(got, dim - 2 * rows, 1)
            before = top_row[...]
            top = jnp.maximum(before, jnp.max(got, axis=0, keepdims=True))
            weight = jnp.exp2(got - top)
            keep = jnp.exp2(before - top)
            top_row[...] = top
            weighted = weight * totals
            new_total = total_row[...] * keep
            for i in range(NX):
                new_total = new_total + weighted[i : i + 1]
            total_row[...] = new_total
            scaled = weight * scales
            numer = total_numer[...] * to_column(keep, rows)
            for i, src in enumerate(sources):
                numer = numer + recv16[src].astype(jnp.int32).astype(jnp.float32) * to_column(
                    scaled[i : i + 1], rows
                )
            total_numer[...] = numer

        @pl.loop(OWNER + 1, LATE)
        def _(zz):
            add(zz)

        add(OWNER, NX - 1)
        add(0)

        @pl.loop(LATE, NZ)
        def _(zz):
            add(zz)

        done = total_numer[...] / to_column(total_row[...], rows)
        finished[x] = done.astype(finished.dtype)
        with jax.named_scope("bcast"):
            for zz in near_z:
                for xx in range(NX):
                    if zz == OWNER:

                        @pl.when(x != xx)
                        def _():
                            near(zz, xx).start()
                    else:
                        near(zz, xx).start()

    def forward(i):
        return remote(finished, finished, send_w, recv_f, x * NZ + column[i])

    with jax.named_scope("fw"):

        @pl.when(owner)
        def _():
            wait_rows(recv_f, kv - 1)

        @pl.when(jnp.logical_not(owner))
        def _():
            wait_rows(recv_f, kv)

    @pl.when(relay)
    def _():
        pl.semaphore_wait(ready, len(column))
        for i in range(len(column)):
            forward(i).start()

    fin_f32[...] = finished[...].astype(jnp.float32).reshape(heads * batch, dim)
    for b in range(batch):
        out_ref[b] = fin_f32[pl.ds(b, heads, stride=batch), :].astype(out_ref.dtype)

    with jax.named_scope("ws"):

        @pl.when(owner)
        def _():
            wait_for(send_p, kv - 1)
            wait_rows(send_f, len(near_z) * NX - 1)

        @pl.when(jnp.logical_not(owner))
        def _():
            wait_for(send_p, kv)

        @pl.when(relay)
        def _():
            wait_rows(send_w, len(column) * kv)


def shards(query_rows, cache_keys, cache_values, page_table, seq_lengths):
    slots, kv, page, dim = cache_keys.shape
    batch, heads, _ = query_rows.shape
    rows = heads // kv * batch
    devices = NX * NZ
    dma = pltpu.SemaphoreType.DMA
    return pl.pallas_call(
        kernel,
        out_shape=jax.ShapeDtypeStruct(query_rows.shape, query_rows.dtype),
        in_specs=[pl.BlockSpec(memory_space=pltpu.HBM)] * 5,
        out_specs=pl.BlockSpec(memory_space=pltpu.VMEM),
        scratch_shapes=[
            pltpu.SMEM(seq_lengths.shape, seq_lengths.dtype),
            pltpu.VMEM(query_rows.shape, query_rows.dtype),
            pltpu.VMEM((batch * heads, dim), jnp.float32),
            pltpu.VMEM((slots, 2, page, dim), cache_keys.dtype),
            pltpu.VMEM((slots, 2, page, dim), cache_keys.dtype),
            pltpu.VMEM((slots, 2, page, dim), cache_values.dtype),
            pltpu.VMEM((slots, 2, page, dim), cache_values.dtype),
            pltpu.VMEM((page_table.shape[0] // page, page), jnp.int32),
            pltpu.VMEM((slots, batch, page), jnp.float32),
            pltpu.VMEM((2 * rows, slots * page), jnp.float32),
            pltpu.VMEM((2 * rows, slots * page), jnp.float32),
            pltpu.VMEM((2 * rows, slots * page), jnp.bfloat16),
            pltpu.VMEM((2 * rows, slots * page), jnp.bfloat16),
            pltpu.VMEM((kv, rows, dim), jnp.int16),
            pltpu.VMEM((kv, 1, dim), jnp.float32),
            pltpu.VMEM((devices, rows, dim), jnp.int16),
            pltpu.VMEM((NX * (rows // 2 + 1), 1, dim), jnp.float32),
            pltpu.VMEM((rows, dim), jnp.float32),
            pltpu.VMEM((1, dim), jnp.float32),
            pltpu.VMEM((1, dim), jnp.float32),
            pltpu.VMEM((kv, rows, dim), query_rows.dtype),
            pltpu.VMEM((heads * batch, dim), jnp.float32),
            dma((3,)),
            dma((3,)),
            dma((3,)),
            dma(()),
            dma((NZ,)),
            dma(()),
            dma(()),
            dma(()),
            pltpu.SemaphoreType.REGULAR,
        ],
        compiler_params=pltpu.CompilerParams(
            collective_id=0, has_side_effects=True, vmem_limit_bytes=40 << 20
        ),
        name="attend",
    )(
        *(
            pltpu.with_memory_space_constraint(a, pltpu.HBM)
            for a in (query_rows, cache_keys, cache_values, page_table.reshape(-1, page), seq_lengths)
        )
    )


def solution(mesh):
    return jax.shard_map(
        shards,
        mesh=mesh,
        in_specs=(
            P("grp", "head", None),
            P(("grp", "seq"), "head", None, None),
            P(("grp", "seq"), "head", None, None),
            P("grp"),
            P("grp"),
        ),
        out_specs=P("grp", "head", None),
        check_vma=False,
    )
```

```python
import functools
import math

import jax
import jax.numpy as jnp
from jax import lax
from jax.experimental import pallas as pl
from jax.experimental.pallas import tpu as pltpu
from jax.sharding import PartitionSpec as P

MESH = pl.DeviceIdType.MESH
NX, NZ = 4, 16
OWNER = 1
NEAR = 3
RELAY = 5
LATE = 13
VERY_LOW = -1e30
LOWEST = -3e38
LEVELS = 32767.0


def remote(src, dst, send, recv, seq):
    return pltpu.make_async_remote_copy(
        src_ref=src,
        dst_ref=dst,
        send_sem=send,
        recv_sem=recv,
        device_id={"seq": seq},
        device_id_type=MESH,
    )


def diagonal(rows, lanes, first):
    lane = lax.broadcasted_iota(jnp.int32, (rows, lanes), 1)
    sub = lax.broadcasted_iota(jnp.int32, (rows, lanes), 0)
    return lane == sub + first


def to_column(row, rows):
    return jnp.sum(jnp.where(diagonal(rows, row.shape[1], 0), row, 0.0), axis=1, keepdims=True)


def kernel(
    q_hbm, k_hbm, v_hbm, table_hbm, len_hbm, out_ref,
    len_buf, q_buf, q_f32, k_buf0, k_buf1, v_buf0, v_buf1, table_buf, bias, scores0, scores1, probs0, probs1,
    numer16, stats, recv16, recv_stats, total_numer, total_row, top_row, finished, fin_f32,
    load_sem, k_sem, v_sem, send_p, recv_p, send_f, recv_f, send_w, ready,
):
    slots, kv, page, dim = k_hbm.shape
    batch, heads, _ = q_hbm.shape
    group = heads // kv
    table_rows = table_hbm.shape[0] // batch
    rows = group * batch
    pairs = [(g, g + 1) for g in range(0, kv, 2)]
    devices = NX * NZ

    load_t = pltpu.make_async_copy(table_hbm, table_buf, load_sem.at[0])
    load_l = pltpu.make_async_copy(len_hbm, len_buf, load_sem.at[1])
    load_q = pltpu.make_async_copy(q_hbm, q_buf, load_sem.at[2])
    k_buf, v_buf, scores, probs = (k_buf0, k_buf1), (v_buf0, v_buf1), (scores0, scores1), (probs0, probs1)
    half = slots // 2

    def loads(source, target, p, sems, parts):
        size = slots // parts
        return [
            pltpu.make_async_copy(
                source.at[pl.ds(i * size, size), pl.ds(2 * p, 2)], target.at[pl.ds(i * size, size)], sems.at[i]
            )
            for i in range(parts)
        ]

    loads_k0 = loads(k_hbm, k_buf0, 0, k_sem.at[pl.ds(0, 2)], 2)
    loads_k1 = loads(k_hbm, k_buf1, 1, k_sem.at[pl.ds(2, 1)], 1)
    loads_v0 = loads(v_hbm, v_buf0, 0, v_sem.at[pl.ds(0, 1)], 1)
    loads_v1 = loads(v_hbm, v_buf1, 1, v_sem.at[pl.ds(1, 2)], 2)

    load_t.start()
    load_l.start()
    load_q.start()
    loads_k0[0].start()
    loads_k0[1].start()
    loads_v0[0].start()

    me = lax.axis_index("seq")
    x, z = me // NZ, me % NZ
    owner = z == OWNER
    relay = z == RELAY
    fed = jnp.logical_and(z > NEAR, jnp.logical_not(relay))
    owners = [g * NZ + OWNER for g in range(kv)]
    column = [zz for zz in range(NEAR + 1, NZ) if zz != RELAY]

    barrier = pltpu.get_barrier_semaphore()

    def signal(sem, other):
        pl.semaphore_signal(sem, inc=1, device_id={"seq": other}, device_id_type=MESH)

    @pl.when(owner)
    def _():
        @pl.loop(1, devices)
        def _(i):
            signal(barrier, (me + i) % devices)

    @pl.when(jnp.logical_not(owner))
    def _():
        for other in owners:
            signal(barrier, other)

    @pl.when(relay)
    def _():
        for zz in column:
            signal(barrier, x * NZ + zz)

    with jax.named_scope("tw"):
        load_t.wait()
        load_l.wait()
        load_q.wait()
    loads_k1[0].start()
    first = me * slots
    lane = lax.broadcasted_iota(jnp.int32, (batch, page), 1)
    sub = lax.broadcasted_iota(jnp.int32, (batch, page), 0)
    length = jnp.zeros((batch, page), jnp.int32)
    for b in range(batch):
        length = jnp.where(sub == b, len_buf[b], length)
    tables = [table_buf[pl.ds(r, batch, stride=table_rows), :] for r in range(table_rows)]
    spans = [(length - page * (lane + page * r)).astype(jnp.float32) for r in range(table_rows)]
    lane_f32 = lane.astype(jnp.float32)
    for s in range(slots):
        found = functools.reduce(
            jnp.add, [jnp.where(t == first + s, n, 0.0) for t, n in zip(tables, spans)]
        )
        live = jnp.sum(found, axis=1, keepdims=True)
        bias[s] = jnp.where(lane_f32 < live, 0.0, VERY_LOW)
    q_f32[...] = q_buf[...].astype(jnp.float32).reshape(batch * heads, dim)

    factor = math.log2(math.e) / math.sqrt(dim)

    def sends(g):
        slot = z * NX + x
        return (
            remote(numer16.at[g], recv16.at[slot], send_p, recv_p.at[z], owners[g]),
            remote(stats.at[g], recv_stats.at[slot], send_p, recv_p.at[z], owners[g]),
        )

    def wait_for(sem, chunks):
        part = recv_stats.at[pl.ds(0, chunks * (rows // 2 + 1))]
        pltpu.make_async_copy(part, part, sem).wait()

    def wait_rows(sem, chunks):
        part = recv16.at[pl.ds(0, chunks)]
        pltpu.make_async_copy(part, part, sem).wait()

    def queries(p):
        blocks = []
        for i, g in enumerate(pairs[p]):
            query = jnp.concatenate(
                [q_f32[pl.ds(group * g + j, batch, stride=heads), :] for j in range(group)], axis=0
            ).astype(jnp.bfloat16)
            empty = jnp.zeros_like(query)
            blocks.append(jnp.concatenate([empty] * i + [query] + [empty] * (1 - i), axis=1))
        return jnp.concatenate(blocks, axis=0)

    def both(buf, s):
        return jnp.concatenate([buf[s : s + 2, i].reshape(2 * page, dim) for i in range(2)], axis=1)

    def score(p, query, s, best):
        got = lax.dot_general(
            query, both(k_buf[p], s), (((1,), (1,)), ((), ())), preferred_element_type=jnp.float32
        )
        for u in range(2):
            add = jnp.concatenate([bias[s + u]] * (2 * group), axis=0)
            now = got[:, u * page : (u + 1) * page] * factor + add
            scores[p][:, (s + u) * page : (s + u + 1) * page] = now
            best = now if best is None else jnp.maximum(best, now)
        return best

    def weigh(p, top, s, total):
        for u in range(s, s + 2):
            w = jnp.exp2(scores[p][:, u * page : (u + 1) * page] - top)
            total = w if total is None else total + w
            probs[p][:, u * page : (u + 1) * page] = w.astype(jnp.bfloat16)
        return total

    def attend(p, s, numers):
        now = jnp.dot(
            probs[p][:, s * page : (s + 2) * page], both(v_buf[p], s), preferred_element_type=jnp.float32
        )
        turn = s // 2 % 2
        numers[turn] = now if numers[turn] is None else numers[turn] + now

    def joined(sums):
        return jnp.maximum(sums[0], LOWEST) + sums[1]

    def finish(p, numers, top, total):
        total = jnp.sum(total, axis=1, keepdims=True)
        for i, g in enumerate(pairs[p]):
            own = slice(i * rows, (i + 1) * rows)
            numer = numers[own, i * dim : (i + 1) * dim]
            largest = jnp.max(jnp.abs(numer), axis=1, keepdims=True)
            steps = numer * (LEVELS / jnp.maximum(largest, 1e-30))
            numer16[g] = jnp.floor(steps + 0.5).astype(jnp.int32).astype(jnp.int16)
            row = sum(
                jnp.where(diagonal(rows, dim, j * rows), c, 0.0)
                for j, c in enumerate((top[own], total[own], largest * (1.0 / LEVELS)))
            )
            stats[g] = jnp.sum(row, axis=0, keepdims=True)

        @pl.when(jnp.logical_not(owner))
        def _():
            with jax.named_scope(f"snd{p}"):
                for g in pairs[p]:
                    for c in sends(g):
                        c.start()

    steps = range(0, slots, 2)
    query0, query1 = queries(0), queries(1)
    with jax.named_scope("bw"):

        @pl.when(fed)
        def _():
            pl.semaphore_wait(barrier, kv + 1)
            signal(ready, x * NZ + RELAY)

        @pl.when(jnp.logical_not(jnp.logical_or(owner, fed)))
        def _():
            pl.semaphore_wait(barrier, kv)

    best0 = None
    for i in range(2):
        with jax.named_scope(f"kw0{i}"):
            loads_k0[i].wait()
        if i == 0:
            loads_v1[0].start()
            loads_v1[1].start()
        for s in range(i * half, (i + 1) * half, 2):
            best0 = score(0, query0, s, best0)
    top0 = jnp.max(best0, axis=1, keepdims=True)
    with jax.named_scope("vw0"):
        loads_v0[0].wait()
    numers0, total0 = [None, None], None
    for s in steps:
        total0 = weigh(0, top0, s, total0)
        attend(0, s, numers0)

    finish(0, joined(numers0), top0, total0)
    with jax.named_scope("kw1"):
        loads_k1[0].wait()
    best1 = None
    for s in steps:
        best1 = score(1, query1, s, best1)
    top1 = jnp.max(best1, axis=1, keepdims=True)
    numers1, total1 = [None, None], None
    for i in range(2):
        with jax.named_scope(f"vw1{i}"):
            loads_v1[i].wait()
        for s in range(i * half, (i + 1) * half, 2):
            total1 = weigh(1, top1, s, total1)
            attend(1, s, numers1)
    finish(1, joined(numers1), top1, total1)

    def near(zz, xx):
        other = xx * NZ + zz
        return remote(
            finished.at[x], finished.at[x], send_f, recv_f, other
        )

    near_z = [*range(NEAR + 1), RELAY]

    @pl.when(owner)
    def _():
        with jax.named_scope("bar"):
            pl.semaphore_wait(barrier, devices - 1)
        for g in range(kv):

            @pl.when(x != g)
            def _():
                for c in sends(g):
                    c.start()

        slot = z * NX + x
        recv16[slot] = numer16[x]
        recv_stats[slot] = stats[x]
        total_numer[...] = jnp.zeros_like(total_numer)
        total_row[...] = jnp.zeros_like(total_row)
        top_row[...] = jnp.full_like(top_row, VERY_LOW)

        def add(zz, chunks=NX):
            sources = [zz * NX + xx for xx in range(NX)]
            with jax.named_scope("rw"):
                wait_for(recv_p.at[zz], chunks)

            got = jnp.concatenate([recv_stats[src] for src in sources] * 2, axis=0)
            totals = pltpu.roll(got, dim - rows, 1)
            scales = pltpu.roll(got, dim - 2 * rows, 1)
            before = top_row[...]
            top = jnp.maximum(before, jnp.max(got, axis=0, keepdims=True))
            weight = jnp.exp2(got - top)
            keep = jnp.exp2(before - top)
            top_row[...] = top
            weighted = weight * totals
            new_total = total_row[...] * keep
            for i in range(NX):
                new_total = new_total + weighted[i : i + 1]
            total_row[...] = new_total
            scaled = weight * scales
            numer = total_numer[...] * to_column(keep, rows)
            for i, src in enumerate(sources):
                numer = numer + recv16[src].astype(jnp.int32).astype(jnp.float32) * to_column(
                    scaled[i : i + 1], rows
                )
            total_numer[...] = numer

        @pl.loop(OWNER + 1, LATE)
        def _(zz):
            add(zz)

        add(OWNER, NX - 1)
        add(0)

        @pl.loop(LATE, NZ)
        def _(zz):
            add(zz)

        done = total_numer[...] / to_column(total_row[...], rows)
        finished[x] = done.astype(finished.dtype)
        with jax.named_scope("bcast"):
            for zz in near_z:
                for xx in range(NX):
                    if zz == OWNER:

                        @pl.when(x != xx)
                        def _():
                            near(zz, xx).start()
                    else:
                        near(zz, xx).start()

    def forward(i):
        return remote(finished, finished, send_w, recv_f, x * NZ + column[i])

    with jax.named_scope("fw"):

        @pl.when(owner)
        def _():
            wait_rows(recv_f, kv - 1)

        @pl.when(jnp.logical_not(owner))
        def _():
            wait_rows(recv_f, kv)

    @pl.when(relay)
    def _():
        pl.semaphore_wait(ready, len(column))
        for i in range(len(column)):
            forward(i).start()

    fin_f32[...] = finished[...].astype(jnp.float32).reshape(heads * batch, dim)
    for b in range(batch):
        out_ref[b] = fin_f32[pl.ds(b, heads, stride=batch), :].astype(out_ref.dtype)

    with jax.named_scope("ws"):

        @pl.when(owner)
        def _():
            wait_for(send_p, kv - 1)
            wait_rows(send_f, len(near_z) * NX - 1)

        @pl.when(jnp.logical_not(owner))
        def _():
            wait_for(send_p, kv)

        @pl.when(relay)
        def _():
            wait_rows(send_w, len(column) * kv)


def shards(query_rows, cache_keys, cache_values, page_table, seq_lengths):
    slots, kv, page, dim = cache_keys.shape
    batch, heads, _ = query_rows.shape
    rows = heads // kv * batch
    devices = NX * NZ
    dma = pltpu.SemaphoreType.DMA
    return pl.pallas_call(
        kernel,
        out_shape=jax.ShapeDtypeStruct(query_rows.shape, query_rows.dtype),
        in_specs=[pl.BlockSpec(memory_space=pltpu.HBM)] * 5,
        out_specs=pl.BlockSpec(memory_space=pltpu.VMEM),
        scratch_shapes=[
            pltpu.SMEM(seq_lengths.shape, seq_lengths.dtype),
            pltpu.VMEM(query_rows.shape, query_rows.dtype),
            pltpu.VMEM((batch * heads, dim), jnp.float32),
            pltpu.VMEM((slots, 2, page, dim), cache_keys.dtype),
            pltpu.VMEM((slots, 2, page, dim), cache_keys.dtype),
            pltpu.VMEM((slots, 2, page, dim), cache_values.dtype),
            pltpu.VMEM((slots, 2, page, dim), cache_values.dtype),
            pltpu.VMEM((page_table.shape[0] // page, page), jnp.int32),
            pltpu.VMEM((slots, batch, page), jnp.float32),
            pltpu.VMEM((2 * rows, slots * page), jnp.float32),
            pltpu.VMEM((2 * rows, slots * page), jnp.float32),
            pltpu.VMEM((2 * rows, slots * page), jnp.bfloat16),
            pltpu.VMEM((2 * rows, slots * page), jnp.bfloat16),
            pltpu.VMEM((kv, rows, dim), jnp.int16),
            pltpu.VMEM((kv, 1, dim), jnp.float32),
            pltpu.VMEM((devices, rows, dim), jnp.int16),
            pltpu.VMEM((NX * (rows // 2 + 1), 1, dim), jnp.float32),
            pltpu.VMEM((rows, dim), jnp.float32),
            pltpu.VMEM((1, dim), jnp.float32),
            pltpu.VMEM((1, dim), jnp.float32),
            pltpu.VMEM((kv, rows, dim), query_rows.dtype),
            pltpu.VMEM((heads * batch, dim), jnp.float32),
            dma((3,)),
            dma((3,)),
            dma((3,)),
            dma(()),
            dma((NZ,)),
            dma(()),
            dma(()),
            dma(()),
            pltpu.SemaphoreType.REGULAR,
        ],
        compiler_params=pltpu.CompilerParams(
            collective_id=0, has_side_effects=True, vmem_limit_bytes=40 << 20
        ),
        name="attend",
    )(
        *(
            pltpu.with_memory_space_constraint(a, pltpu.HBM)
            for a in (query_rows, cache_keys, cache_values, page_table.reshape(-1, page), seq_lengths)
        )
    )


def solution(mesh):
    return jax.shard_map(
        shards,
        mesh=mesh,
        in_specs=(
            P("grp", "head", None),
            P(("grp", "seq"), "head", None, None),
            P(("grp", "seq"), "head", None, None),
            P("grp"),
            P("grp"),
        ),
        out_specs=P("grp", "head", None),
        check_vma=False,
    )
```

```python
import functools
import math

import jax
import jax.numpy as jnp
from jax import lax
from jax.experimental import pallas as pl
from jax.experimental.pallas import tpu as pltpu
from jax.sharding import PartitionSpec as P

MESH = pl.DeviceIdType.MESH
NX, NZ = 4, 16
OWNER = 1
NEAR = 3
RELAY = 5
LATE = 13
VERY_LOW = -1e30
LOWEST = -3e38
LEVELS = 32767.0


def remote(src, dst, send, recv, seq):
    return pltpu.make_async_remote_copy(
        src_ref=src,
        dst_ref=dst,
        send_sem=send,
        recv_sem=recv,
        device_id={"seq": seq},
        device_id_type=MESH,
    )


def diagonal(rows, lanes, first):
    lane = lax.broadcasted_iota(jnp.int32, (rows, lanes), 1)
    sub = lax.broadcasted_iota(jnp.int32, (rows, lanes), 0)
    return lane == sub + first


def to_column(row, rows):
    return jnp.sum(jnp.where(diagonal(rows, row.shape[1], 0), row, 0.0), axis=1, keepdims=True)


def kernel(
    q_hbm, k_hbm, v_hbm, table_hbm, len_hbm, out_ref,
    len_buf, q_buf, q_f32, k_buf0, k_buf1, v_buf0, v_buf1, table_buf, bias, scores0, scores1, probs0, probs1,
    numer16, stats, recv16, recv_stats, total_numer, total_row, top_row, finished, fin_f32,
    load_sem, k_sem, v_sem, send_p, recv_p, send_f, recv_f, send_w, ready,
):
    slots, kv, page, dim = k_hbm.shape
    batch, heads, _ = q_hbm.shape
    group = heads // kv
    table_rows = table_hbm.shape[0] // batch
    rows = group * batch
    pairs = [(g, g + 1) for g in range(0, kv, 2)]
    devices = NX * NZ

    load_t = pltpu.make_async_copy(table_hbm, table_buf, load_sem.at[0])
    load_l = pltpu.make_async_copy(len_hbm, len_buf, load_sem.at[1])
    load_q = pltpu.make_async_copy(q_hbm, q_buf, load_sem.at[2])
    k_buf, v_buf, scores, probs = (k_buf0, k_buf1), (v_buf0, v_buf1), (scores0, scores1), (probs0, probs1)
    half = slots // 2

    def loads(source, target, p, sems, parts):
        size = slots // parts
        return [
            pltpu.make_async_copy(
                source.at[pl.ds(i * size, size), pl.ds(2 * p, 2)], target.at[pl.ds(i * size, size)], sems.at[i]
            )
            for i in range(parts)
        ]

    loads_k0 = loads(k_hbm, k_buf0, 0, k_sem.at[pl.ds(0, 2)], 2)
    loads_k1 = loads(k_hbm, k_buf1, 1, k_sem.at[pl.ds(2, 1)], 1)
    loads_v0 = loads(v_hbm, v_buf0, 0, v_sem.at[pl.ds(0, 1)], 1)
    loads_v1 = loads(v_hbm, v_buf1, 1, v_sem.at[pl.ds(1, 2)], 2)

    load_t.start()
    load_l.start()
    load_q.start()
    loads_k0[0].start()
    loads_k0[1].start()
    loads_v0[0].start()

    me = lax.axis_index("seq")
    x, z = me // NZ, me % NZ
    owner = z == OWNER
    relay = z == RELAY
    fed = jnp.logical_and(z > NEAR, jnp.logical_not(relay))
    owners = [g * NZ + OWNER for g in range(kv)]
    column = [zz for zz in range(NEAR + 1, NZ) if zz != RELAY]

    barrier = pltpu.get_barrier_semaphore()

    def signal(sem, other):
        pl.semaphore_signal(sem, inc=1, device_id={"seq": other}, device_id_type=MESH)

    @pl.when(owner)
    def _():
        @pl.loop(1, devices)
        def _(i):
            signal(barrier, (me + i) % devices)

    @pl.when(jnp.logical_not(owner))
    def _():
        for other in owners:
            signal(barrier, other)

    @pl.when(relay)
    def _():
        for zz in column:
            signal(barrier, x * NZ + zz)

    with jax.named_scope("tw"):
        load_t.wait()
        load_l.wait()
        load_q.wait()
    loads_k1[0].start()
    first = me * slots
    lane = lax.broadcasted_iota(jnp.int32, (batch, page), 1)
    sub = lax.broadcasted_iota(jnp.int32, (batch, page), 0)
    length = jnp.zeros((batch, page), jnp.int32)
    for b in range(batch):
        length = jnp.where(sub == b, len_buf[b], length)
    tables = [table_buf[pl.ds(r, batch, stride=table_rows), :] for r in range(table_rows)]
    spans = [(length - page * (lane + page * r)).astype(jnp.float32) for r in range(table_rows)]
    lane_f32 = lane.astype(jnp.float32)
    for s in range(slots):
        found = functools.reduce(
            jnp.add, [jnp.where(t == first + s, n, 0.0) for t, n in zip(tables, spans)]
        )
        live = jnp.sum(found, axis=1, keepdims=True)
        bias[s] = jnp.where(lane_f32 < live, 0.0, VERY_LOW)
    q_f32[...] = q_buf[...].astype(jnp.float32).reshape(batch * heads, dim)

    factor = math.log2(math.e) / math.sqrt(dim)

    def sends(g):
        slot = z * NX + x
        return (
            remote(numer16.at[g], recv16.at[slot], send_p, recv_p.at[z], owners[g]),
            remote(stats.at[g], recv_stats.at[slot], send_p, recv_p.at[z], owners[g]),
        )

    def wait_for(sem, chunks):
        part = recv_stats.at[pl.ds(0, chunks * (rows // 2 + 1))]
        pltpu.make_async_copy(part, part, sem).wait()

    def wait_rows(sem, chunks):
        part = recv16.at[pl.ds(0, chunks)]
        pltpu.make_async_copy(part, part, sem).wait()

    def queries(p):
        blocks = []
        for i, g in enumerate(pairs[p]):
            query = jnp.concatenate(
                [q_f32[pl.ds(group * g + j, batch, stride=heads), :] for j in range(group)], axis=0
            ).astype(jnp.bfloat16)
            empty = jnp.zeros_like(query)
            blocks.append(jnp.concatenate([empty] * i + [query] + [empty] * (1 - i), axis=1))
        return jnp.concatenate(blocks, axis=0)

    def both(buf, s):
        return jnp.concatenate([buf[s : s + 2, i].reshape(2 * page, dim) for i in range(2)], axis=1)

    def score(p, query, s, best):
        got = lax.dot_general(
            query, both(k_buf[p], s), (((1,), (1,)), ((), ())), preferred_element_type=jnp.float32
        )
        for u in range(2):
            add = jnp.concatenate([bias[s + u]] * (2 * group), axis=0)
            now = got[:, u * page : (u + 1) * page] * factor + add
            scores[p][:, (s + u) * page : (s + u + 1) * page] = now
            best = now if best is None else jnp.maximum(best, now)
        return best

    def weigh(p, top, s, total):
        for u in range(s, s + 2):
            w = jnp.exp2(scores[p][:, u * page : (u + 1) * page] - top)
            total = w if total is None else total + w
            probs[p][:, u * page : (u + 1) * page] = w.astype(jnp.bfloat16)
        return total

    def attend(p, s, numers):
        now = jnp.dot(
            probs[p][:, s * page : (s + 2) * page], both(v_buf[p], s), preferred_element_type=jnp.float32
        )
        turn = s // 2 % 2
        numers[turn] = now if numers[turn] is None else numers[turn] + now

    def joined(sums):
        return jnp.maximum(sums[0], LOWEST) + sums[1]

    def finish(p, numers, top, total):
        total = jnp.sum(total, axis=1, keepdims=True)
        for i, g in enumerate(pairs[p]):
            own = slice(i * rows, (i + 1) * rows)
            numer = numers[own, i * dim : (i + 1) * dim]
            largest = jnp.max(jnp.abs(numer), axis=1, keepdims=True)
            steps = numer * (LEVELS / jnp.maximum(largest, 1e-30))
            numer16[g] = jnp.floor(steps + 0.5).astype(jnp.int32).astype(jnp.int16)
            row = sum(
                jnp.where(diagonal(rows, dim, j * rows), c, 0.0)
                for j, c in enumerate((top[own], total[own], largest * (1.0 / LEVELS)))
            )
            stats[g] = jnp.sum(row, axis=0, keepdims=True)

        @pl.when(jnp.logical_not(owner))
        def _():
            with jax.named_scope(f"snd{p}"):
                for g in pairs[p] if p else pairs[p][::-1]:
                    for c in sends(g):
                        c.start()

    steps = range(0, slots, 2)
    query0, query1 = queries(0), queries(1)
    best0 = None
    for i in range(2):
        with jax.named_scope(f"kw0{i}"):
            loads_k0[i].wait()
        if i == 0:
            loads_v1[0].start()
            loads_v1[1].start()
        for s in range(i * half, (i + 1) * half, 2):
            best0 = score(0, query0, s, best0)
    top0 = jnp.max(best0, axis=1, keepdims=True)
    with jax.named_scope("vw0"):
        loads_v0[0].wait()
    numers0, total0 = [None, None], None
    for s in steps:
        total0 = weigh(0, top0, s, total0)
        attend(0, s, numers0)

    with jax.named_scope("bw"):

        @pl.when(fed)
        def _():
            pl.semaphore_wait(barrier, kv + 1)
            signal(ready, x * NZ + RELAY)

        @pl.when(jnp.logical_not(jnp.logical_or(owner, fed)))
        def _():
            pl.semaphore_wait(barrier, kv)

    finish(0, joined(numers0), top0, total0)
    with jax.named_scope("kw1"):
        loads_k1[0].wait()
    best1 = None
    for s in steps:
        best1 = score(1, query1, s, best1)
    top1 = jnp.max(best1, axis=1, keepdims=True)
    numers1, total1 = [None, None], None
    for i in range(2):
        with jax.named_scope(f"vw1{i}"):
            loads_v1[i].wait()
        for s in range(i * half, (i + 1) * half, 2):
            total1 = weigh(1, top1, s, total1)
            attend(1, s, numers1)
    finish(1, joined(numers1), top1, total1)

    def near(zz, xx):
        other = xx * NZ + zz
        return remote(
            finished.at[x], finished.at[x], send_f, recv_f, other
        )

    near_z = [*range(NEAR + 1), RELAY]

    @pl.when(owner)
    def _():
        with jax.named_scope("bar"):
            pl.semaphore_wait(barrier, devices - 1)
        for g in range(kv):

            @pl.when(x != g)
            def _():
                for c in sends(g):
                    c.start()

        slot = z * NX + x
        recv16[slot] = numer16[x]
        recv_stats[slot] = stats[x]
        total_numer[...] = jnp.zeros_like(total_numer)
        total_row[...] = jnp.zeros_like(total_row)
        top_row[...] = jnp.full_like(top_row, VERY_LOW)

        def add(zz, chunks=NX):
            sources = [zz * NX + xx for xx in range(NX)]
            with jax.named_scope("rw"):
                wait_for(recv_p.at[zz], chunks)

            got = jnp.concatenate([recv_stats[src] for src in sources] * 2, axis=0)
            totals = pltpu.roll(got, dim - rows, 1)
            scales = pltpu.roll(got, dim - 2 * rows, 1)
            before = top_row[...]
            top = jnp.maximum(before, jnp.max(got, axis=0, keepdims=True))
            weight = jnp.exp2(got - top)
            keep = jnp.exp2(before - top)
            top_row[...] = top
            weighted = weight * totals
            new_total = total_row[...] * keep
            for i in range(NX):
                new_total = new_total + weighted[i : i + 1]
            total_row[...] = new_total
            scaled = weight * scales
            numer = total_numer[...] * to_column(keep, rows)
            for i, src in enumerate(sources):
                numer = numer + recv16[src].astype(jnp.int32).astype(jnp.float32) * to_column(
                    scaled[i : i + 1], rows
                )
            total_numer[...] = numer

        @pl.loop(OWNER + 1, LATE)
        def _(zz):
            add(zz)

        add(OWNER, NX - 1)
        add(0)

        @pl.loop(LATE, NZ)
        def _(zz):
            add(zz)

        done = total_numer[...] / to_column(total_row[...], rows)
        finished[x] = done.astype(finished.dtype)
        with jax.named_scope("bcast"):
            for zz in near_z:
                for xx in range(NX):
                    if zz == OWNER:

                        @pl.when(x != xx)
                        def _():
                            near(zz, xx).start()
                    else:
                        near(zz, xx).start()

    def forward(i):
        return remote(finished, finished, send_w, recv_f, x * NZ + column[i])

    with jax.named_scope("fw"):

        @pl.when(owner)
        def _():
            wait_rows(recv_f, kv - 1)

        @pl.when(jnp.logical_not(owner))
        def _():
            wait_rows(recv_f, kv)

    @pl.when(relay)
    def _():
        pl.semaphore_wait(ready, len(column))
        for i in range(len(column)):
            forward(i).start()

    fin_f32[...] = finished[...].astype(jnp.float32).reshape(heads * batch, dim)
    for b in range(batch):
        out_ref[b] = fin_f32[pl.ds(b, heads, stride=batch), :].astype(out_ref.dtype)

    with jax.named_scope("ws"):

        @pl.when(owner)
        def _():
            wait_for(send_p, kv - 1)
            wait_rows(send_f, len(near_z) * NX - 1)

        @pl.when(jnp.logical_not(owner))
        def _():
            wait_for(send_p, kv)

        @pl.when(relay)
        def _():
            wait_rows(send_w, len(column) * kv)


def shards(query_rows, cache_keys, cache_values, page_table, seq_lengths):
    slots, kv, page, dim = cache_keys.shape
    batch, heads, _ = query_rows.shape
    rows = heads // kv * batch
    devices = NX * NZ
    dma = pltpu.SemaphoreType.DMA
    return pl.pallas_call(
        kernel,
        out_shape=jax.ShapeDtypeStruct(query_rows.shape, query_rows.dtype),
        in_specs=[pl.BlockSpec(memory_space=pltpu.HBM)] * 5,
        out_specs=pl.BlockSpec(memory_space=pltpu.VMEM),
        scratch_shapes=[
            pltpu.SMEM(seq_lengths.shape, seq_lengths.dtype),
            pltpu.VMEM(query_rows.shape, query_rows.dtype),
            pltpu.VMEM((batch * heads, dim), jnp.float32),
            pltpu.VMEM((slots, 2, page, dim), cache_keys.dtype),
            pltpu.VMEM((slots, 2, page, dim), cache_keys.dtype),
            pltpu.VMEM((slots, 2, page, dim), cache_values.dtype),
            pltpu.VMEM((slots, 2, page, dim), cache_values.dtype),
            pltpu.VMEM((page_table.shape[0] // page, page), jnp.int32),
            pltpu.VMEM((slots, batch, page), jnp.float32),
            pltpu.VMEM((2 * rows, slots * page), jnp.float32),
            pltpu.VMEM((2 * rows, slots * page), jnp.float32),
            pltpu.VMEM((2 * rows, slots * page), jnp.bfloat16),
            pltpu.VMEM((2 * rows, slots * page), jnp.bfloat16),
            pltpu.VMEM((kv, rows, dim), jnp.int16),
            pltpu.VMEM((kv, 1, dim), jnp.float32),
            pltpu.VMEM((devices, rows, dim), jnp.int16),
            pltpu.VMEM((NX * (rows // 2 + 1), 1, dim), jnp.float32),
            pltpu.VMEM((rows, dim), jnp.float32),
            pltpu.VMEM((1, dim), jnp.float32),
            pltpu.VMEM((1, dim), jnp.float32),
            pltpu.VMEM((kv, rows, dim), query_rows.dtype),
            pltpu.VMEM((heads * batch, dim), jnp.float32),
            dma((3,)),
            dma((3,)),
            dma((3,)),
            dma(()),
            dma((NZ,)),
            dma(()),
            dma(()),
            dma(()),
            pltpu.SemaphoreType.REGULAR,
        ],
        compiler_params=pltpu.CompilerParams(
            collective_id=0, has_side_effects=True, vmem_limit_bytes=40 << 20
        ),
        name="attend",
    )(
        *(
            pltpu.with_memory_space_constraint(a, pltpu.HBM)
            for a in (query_rows, cache_keys, cache_values, page_table.reshape(-1, page), seq_lengths)
        )
    )


def solution(mesh):
    return jax.shard_map(
        shards,
        mesh=mesh,
        in_specs=(
            P("grp", "head", None),
            P(("grp", "seq"), "head", None, None),
            P(("grp", "seq"), "head", None, None),
            P("grp"),
            P("grp"),
        ),
        out_specs=P("grp", "head", None),
        check_vma=False,
    )
```
